256 devices in a mesh: tm: 8 (over x, core), space: 32 (over y, z).
Axes of the slice: x: 4, y: 4, z: 8, core: 2. Of those that a mesh axis runs over, the one named last changes fastest.
Arguments:
- water_depth: float32 [96, 16, 128], P('space'), may hold values from 0.7 to 1.4
- momentum: float32 [96, 2, 16, 128], P('space'), may hold values from -0.6 to 0.6
- slot_live: int32 [96], P('space'), may hold values from 0 to 1, as said below
- neighbours: int32 [96, 2], P('space'), may hold values from 0 to 3, as said below
Outputs:
- slice_ends: float32 [8, 96, 3, 16, 128], P('tm', 'space')
The draws below stay inside these ranges and needn't reach their ends.
Inputs may be any that keep to these rules, and one draw needn't show every extreme that they name: `slot_live`: every owner's 3 consecutive slots hold between 1 and 3 live blocks; owners 2p and 2p + 1 together hold exactly 4 live blocks, and some owner holds 3. `neighbours`: the live blocks of each owner form one run along the channel, and the runs of owners 0, 1, 2 and so on follow one another around the periodic channel. For a live slot, entry 0 names the slot of the same owner holding the block to the west and entry 1 the one to the east, or 3 where that block belongs to the previous (west) or next (east) owner; each owner has exactly one live slot with entry 0 equal to 3 and one with entry 1 equal to 3. A dead slot names itself in both entries.
All inputs are finite; a program needn't handle non-finite values.
Results may differ from the reference program's by a relative error of at most 0.00002.
Values sent between devices are 32-bit elements; how exact they have to be, the bound alone decides.
A program may use at most 64 MiB of HBM per device.

```python
import jax
import jax.numpy as jnp
from jax import lax

BS = 128
BY = 16
SUB = 3
KITER = 2
BLK_DEV = 3
SLOTS = 96
N_TM = 8


def block_layout(key):
    owners = SLOTS // BLK_DEV
    pair_count = owners // 2
    balanced = (BLK_DEV + 1) // 2
    leading = jax.random.randint(jax.random.fold_in(key, 101), (pair_count,), 1, 2 * balanced)
    fullest = jax.random.randint(jax.random.fold_in(key, 102), (), 0, pair_count)
    leading = jnp.where(jnp.arange(pair_count) == fullest, 2 * balanced - 1, leading)
    swapped = jax.random.randint(jax.random.fold_in(key, 103), (pair_count,), 0, 2)
    first_count = jnp.where(swapped == 1, 2 * balanced - leading, leading)
    live_count = jnp.stack([first_count, 2 * balanced - first_count], axis=1).reshape(owners)
    scores = jax.random.randint(jax.random.fold_in(key, 104), (owners, BLK_DEV), 0, 65536)
    run_order = jnp.argsort(scores * BLK_DEV + jnp.arange(BLK_DEV)[None, :], axis=1).astype(jnp.int32)
    position = jnp.argsort(run_order, axis=1).astype(jnp.int32)
    live_slot = position < live_count[:, None]
    own_slot = jnp.broadcast_to(jnp.arange(BLK_DEV, dtype=jnp.int32)[None, :], (owners, BLK_DEV))
    preceding = jnp.take_along_axis(run_order, jnp.maximum(position - 1, 0), axis=1)
    following = jnp.take_along_axis(run_order, jnp.minimum(position + 1, BLK_DEV - 1), axis=1)
    west_slot = jnp.where(position > 0, preceding, BLK_DEV)
    east_slot = jnp.where(position < live_count[:, None] - 1, following, BLK_DEV)
    west_slot = jnp.where(live_slot, west_slot, own_slot).astype(jnp.int32)
    east_slot = jnp.where(live_slot, east_slot, own_slot).astype(jnp.int32)
    return (live_slot.astype(jnp.int32).reshape(SLOTS), jnp.stack([west_slot, east_slot], axis=-1).reshape(SLOTS, 2))


def draw_slot_live(key, part):
    return block_layout(key)[0]


def draw_neighbours(key, part):
    return block_layout(key)[1]


def draw_water_depth(key, part):
    rough = jax.random.uniform(jax.random.fold_in(key, 201), (SLOTS, BY, BS), jnp.float32)
    return (0.7 + 0.7 * rough).astype(jnp.float32)


def shard_levels(stream_key, extent, cuts, low, top_value):
    gain, own = 1.0, jax.random.fold_in(stream_key, 6)
    for dim, shards_of in cuts:
        steps = jnp.exp(jax.random.uniform(jax.random.fold_in(own, dim), (shards_of,), jnp.float32, low / len(cuts), top_value / len(cuts)))
        gain = gain * jnp.repeat(steps, extent[dim] // shards_of).reshape([-1 if axis == dim else 1 for axis in range(len(extent))])
    return gain


def centred(stream_key, shape, spread, reach, cuts=(), kind=jnp.bfloat16):
    result = spread * jax.random.normal(stream_key, shape, jnp.float32)
    if cuts:
        result = result * shard_levels(stream_key, shape, cuts, -0.22, 0.18)
    return jnp.clip(result, -reach, reach).astype(kind)


def setup_inputs(seed: int = 0) -> dict:
    key_list = jax.random.split(jax.random.key(seed), 5)
    return {
        "water_depth": draw_water_depth(jax.random.fold_in(key_list[4], 71), 0),
        "momentum": centred(key_list[1], (SLOTS, 2, BY, BS), 0.15, 0.6, ((0, 32),), jnp.float32),
        "slot_live": draw_slot_live(jax.random.fold_in(key_list[4], 71), 0),
        "neighbours": draw_neighbours(jax.random.fold_in(key_list[4], 71), 0),
    }


GRAVITY = 1.0
TIME_STEP = 0.15

def fluxes(fields, along_ratio, across_ratio):
    height = fields[0]
    drift_along = fields[1] / height
    drift_across = fields[2] / height
    celerity = jnp.sqrt(GRAVITY * height)
    pressure = 0.5 * GRAVITY * height * height
    flux_along = jnp.stack([fields[1], fields[1] * drift_along + pressure, fields[2] * drift_along])
    signal_along = jnp.abs(drift_along) + celerity
    face_along = 0.5 * (flux_along[:, :, :-1] + flux_along[:, :, 1:]) - 0.5 * jnp.maximum(signal_along[:, :-1], signal_along[:, 1:]) * (fields[:, :, 1:] - fields[:, :, :-1])
    interior = fields[:, :, 1:-1]
    flux_across = jnp.stack([fields[2], fields[1] * drift_across, fields[2] * drift_across + pressure])[:, :, 1:-1]
    signal_across = (jnp.abs(drift_across) + celerity)[:, 1:-1]
    mirror = jnp.array([1.0, 1.0, -1.0], dtype=jnp.float32)[:, None, None]
    padded = jnp.concatenate([interior[:, :1] * mirror, interior, interior[:, -1:] * mirror], axis=1)
    padded_flux = jnp.concatenate([-flux_across[:, :1] * mirror, flux_across, -flux_across[:, -1:] * mirror], axis=1)
    padded_signal = jnp.concatenate([signal_across[:1], signal_across, signal_across[-1:]], axis=0)
    face_across = 0.5 * (padded_flux[:, :-1] + padded_flux[:, 1:]) - 0.5 * jnp.maximum(padded_signal[:-1], padded_signal[1:]) * (padded[:, 1:] - padded[:, :-1])
    return -along_ratio * (face_along[:, :, 1:] - face_along[:, :, :-1]) - across_ratio * (face_across[:, 1:] - face_across[:, :-1])

def heun_step(fields, along_ratio, across_ratio):
    predictor = fields[:, :, 1:-1] + fluxes(fields, along_ratio, across_ratio)
    return 0.5 * (fields[:, :, 2:-2] + predictor[:, :, 1:-1] + fluxes(predictor, along_ratio, across_ratio))

def fine_block(fields):
    for substep in range(SUB):
        fields = heun_step(fields, TIME_STEP, TIME_STEP)
    return fields

def coarse_block(fields):
    return heun_step(fields, TIME_STEP * SUB, TIME_STEP * SUB / 3.0)

def restrict(fields):
    return 0.5 * (fields[..., 0::2, :] + fields[..., 1::2, :])

def prolong(fields):
    return jnp.repeat(fields, 2, axis=-2)

def links(slot_live, neighbours):
    total = slot_live.shape[0]
    owners = total // BLK_DEV
    slot_ids = jnp.arange(total, dtype=jnp.int32)
    owner_id = slot_ids // BLK_DEV
    live_slot = slot_live == 1
    first_block = jnp.logical_and(neighbours[:, 0] == BLK_DEV, live_slot)
    last_block = jnp.logical_and(neighbours[:, 1] == BLK_DEV, live_slot)
    first_index = lax.optimization_barrier(jnp.sum(jnp.where(first_block, slot_ids, 0).reshape(owners, BLK_DEV), axis=1)).astype(jnp.int32)
    last_index = lax.optimization_barrier(jnp.sum(jnp.where(last_block, slot_ids, 0).reshape(owners, BLK_DEV), axis=1)).astype(jnp.int32)
    prior_owner = (owner_id + owners - 1) % owners
    next_owner = (owner_id + 1) % owners
    west_slot = jnp.where(neighbours[:, 0] < BLK_DEV, owner_id * BLK_DEV + neighbours[:, 0], last_index[prior_owner])
    east_slot = jnp.where(neighbours[:, 1] < BLK_DEV, owner_id * BLK_DEV + neighbours[:, 1], first_index[next_owner])
    return (west_slot.astype(jnp.int32), east_slot.astype(jnp.int32))

def extend(fields, west_slot, east_slot, rim_width):
    west_rim = jnp.take(fields[..., -rim_width:], west_slot, axis=0)
    east_rim = jnp.take(fields[..., :rim_width], east_slot, axis=0)
    return jnp.concatenate([west_rim, fields, east_rim], axis=-1)

def reference(water_depth, momentum, slot_live, neighbours):
    initial = jnp.concatenate([water_depth[:, None], momentum], axis=1)
    west_slot, east_slot = links(slot_live, neighbours)

    def coarse_all(fields):
        return jax.vmap(coarse_block)(extend(fields, west_slot, east_slot, 2))

    def fine_all(fields):
        return lax.map(fine_block, extend(fields, west_slot, east_slot, 2 * SUB))
    coarse_start = restrict(initial)
    previous = []
    slice_start = [initial]
    current = coarse_start
    for position in range(N_TM):
        propagated = coarse_all(current)
        previous.append(propagated)
        current = propagated
        if position + 1 < N_TM:
            slice_start.append(prolong(current))
    slice_end = []
    for sweep in range(KITER):
        refined = [fine_all(slice_start[position]) for position in range(N_TM)]
        renewed = []
        current = coarse_start
        for position in range(N_TM):
            propagated = coarse_all(current)
            renewed.append(propagated)
            current = propagated + (restrict(refined[position]) - previous[position])
        slice_end = [prolong(renewed[position]) + refined[position] - prolong(previous[position]) for position in range(N_TM)]
        slice_start = [initial] + slice_end[:-1]
        previous = renewed
    live_mask = (slot_live == 1)[:, None, None, None]
    return jnp.stack([jnp.where(live_mask, ending, 0.0) for ending in slice_end])
```

```python
import functools

import jax
import jax.numpy as jnp
from jax import lax
from jax.experimental import pallas as pl
from jax.experimental.pallas import tpu as pltpu
from jax.sharding import PartitionSpec as P

SUB = 3
TIME_STEP = 0.15
ROWS = 16
HALF = 8
LANES = 128
MESH = pl.DeviceIdType.MESH


def pick(index, values):
    result = values[-1]
    for i in range(len(values) - 2, -1, -1):
        result = jnp.where(index == i, values[i], result)
    return result


def derived(h, m, n):
    r = lax.rsqrt(h)
    c = h * r
    inv = r * r
    u = m * inv
    q = n * inv
    p = 0.5 * h * h
    f1 = m * u + p
    f2 = n * u
    g2 = n * q + p
    sx = jnp.abs(u) + c
    sy = jnp.abs(q) + c
    return f1, f2, g2, sx, sy


def faces(a_v, b_v, a_f, b_f, a_s, b_s):
    top = jnp.maximum(a_s, b_s)
    return [(fa + fb) - top * (vb - va) for va, vb, fa, fb in zip(a_v, b_v, a_f, b_f)]


def east(x):
    return pltpu.roll(x, LANES - 1, 1)


def west(x):
    return pltpu.roll(x, 1, 1)


def coarse_rhs(v, row):
    h, m, n = v
    f1, f2, g2, sx, sy = derived(h, m, n)
    fx, fy = (m, f1, f2), (n, f2, g2)
    ve = [east(x) for x in v]
    wx = faces(v, ve, fx, (ve[1], east(f1), east(f2)), sx, east(sx))
    dx = [w - west(w) for w in wx]
    up = lambda x: pltpu.roll(x, HALF - 1, 0)
    down = lambda x: pltpu.roll(x, 1, 0)
    vn = [up(x) for x in v]
    f2n = up(f2)
    wy = faces(v, vn, fy, (vn[2], f2n, up(g2)), sy, up(sy))
    last, first = row == HALF - 1, row == 0
    sn = sy * n
    zero = jnp.zeros_like(h)
    high = [jnp.where(last, w, x) for w, x in zip((zero, zero, 2.0 * (g2 + sn)), wy)]
    low = [jnp.where(first, w, down(x)) for w, x in zip((zero, zero, 2.0 * (g2 - sn)), wy)]
    a, b = -0.5 * TIME_STEP * SUB, -0.5 * TIME_STEP
    return [a * x + b * (y - z) for x, y, z in zip(dx, high, low)]


def coarse(v, row):
    k1 = coarse_rhs(v, row)
    v1 = [x + k for x, k in zip(v, k1)]
    k2 = coarse_rhs(v1, row)
    return [0.5 * ((x + y) + k) for x, y, k in zip(v, v1, k2)]


def fine_pass(load, emit):
    here = load(0)
    f1, f2, g2, sx, sy = derived(*here)
    low = [None, None, 2.0 * (g2 - sy * here[2])]
    for j in range(ROWS):
        if j + 1 < ROWS:
            above = load(j + 1)
            f1a, f2a, g2a, sxa, sya = derived(*above)
            high = faces(here, above, (here[2], f2, g2), (above[2], f2a, g2a), sy, sya)
        else:
            high = [None, None, 2.0 * (g2 + sy * here[2])]
        ve = [east(x) for x in here]
        wx = faces(here, ve, (here[1], f1, f2), (ve[1], east(f1), east(f2)), sx, east(sx))
        diff = []
        for w, hi, lo in zip(wx, high, low):
            d = w - west(w)
            if hi is not None:
                d = d + hi
            if lo is not None:
                d = d - lo
            diff.append(d)
        emit(j, here, diff)
        if j + 1 < ROWS:
            here, f1, f2, g2, sx, sy, low = above, f1a, f2a, g2a, sxa, sya, high


def fine(state, mid):
    def at(ref, j):
        return [ref[f, HALF * j : HALF * j + HALF, :] for f in range(3)]

    def put(ref, j, v):
        for f in range(3):
            ref[f, HALF * j : HALF * j + HALF, :] = v[f]

    def first(j, v, d):
        put(mid, j, [x - (0.5 * TIME_STEP) * y for x, y in zip(v, d)])

    def second(j, v1, d):
        v = at(state, j)
        put(state, j, [0.5 * (x + y) - (0.25 * TIME_STEP) * z for x, y, z in zip(v, v1, d)])

    def step(_, carry):
        fine_pass(lambda j: at(state, j), first)
        fine_pass(lambda j: at(mid, j), second)
        return carry

    lax.fori_loop(0, SUB, step, 0)


def kernel(
    n_tm, owners, seg,
    live_ref, nb_ref, depth_ref, mom_ref, out_ref,
    loc, edge, got, state, mid, delta, ga, ka, send, recv, run,
    in_sem, edge_send, edge_recv, tm_send, tm_recv,
):
    me = lax.axis_index("tm")
    own = lax.axis_index("space")
    east_owner = lax.rem(own + 1, owners)
    west_owner = lax.rem(own + owners - 1, owners)
    blocks = loc.shape[0]

    in_copies = [
        pltpu.make_async_copy(depth_ref, loc.at[:, 0], in_sem.at[0]),
        pltpu.make_async_copy(mom_ref, loc.at[:, 1:3], in_sem.at[1]),
    ]
    for c in in_copies:
        c.start()

    barrier = pltpu.get_barrier_semaphore()
    for o in (west_owner, east_owner):
        pl.semaphore_signal(barrier, inc=1, device_id=(me, o), device_id_type=MESH)
    for d in range(1, n_tm):
        peer = lax.rem(me + d, n_tm)
        pl.semaphore_signal(barrier, inc=1, device_id=(peer, own), device_id_type=MESH)

    lives = [live_ref[b] == 1 for b in range(blocks)]
    wests = [nb_ref[b, 0] for b in range(blocks)]
    easts = [nb_ref[b, 1] for b in range(blocks)]
    count = jnp.int32(0)
    first = jnp.int32(0)
    final = jnp.int32(0)
    for b in range(blocks):
        count = count + jnp.where(lives[b], 1, 0)
        first = first + jnp.where(jnp.logical_and(lives[b], wests[b] == blocks), b, 0)
        final = final + jnp.where(jnp.logical_and(lives[b], easts[b] == blocks), b, 0)
    order = [first]
    for _ in range(blocks - 1):
        order.append(jnp.minimum(pick(order[-1], easts), blocks - 1))

    for c in in_copies:
        c.wait()
    edge[0] = loc[first]
    edge[1] = loc[final]
    pl.semaphore_wait(barrier, n_tm + 1)
    halo = [
        pltpu.make_async_remote_copy(
            src_ref=edge.at[i], dst_ref=got.at[i], send_sem=edge_send.at[i], recv_sem=edge_recv.at[i],
            device_id=(me, o), device_id_type=MESH,
        )
        for i, o in ((0, west_owner), (1, east_owner))
    ]
    for c in halo:
        c.start()

    pad = (LANES - seg) // 2
    begin = seg * me + (LANES - pad)
    place = begin // LANES - 1
    offset = begin % LANES
    lane = lax.broadcasted_iota(jnp.int32, (HALF, LANES), 1)
    row = lax.broadcasted_iota(jnp.int32, (HALF, LANES), 0)
    left = lane >= offset

    for c in halo:
        c.wait()

    def source(position):
        slot = pick(position, order)
        return slot, position < 0, position >= count

    slot_a, west_a, east_a = source(place)
    slot_b, west_b, east_b = source(place + 1)
    slot_a = jnp.clip(slot_a, 0, blocks - 1)
    slot_b = jnp.clip(slot_b, 0, blocks - 1)
    for f in range(3):
        for half in range(2):
            rows = pl.ds(HALF * half, HALF)
            from_east, from_west = got[0, f, rows, :], got[1, f, rows, :]
            xa = jnp.where(west_a, from_west, jnp.where(east_a, from_east, loc[slot_a, f, rows, :]))
            xb = jnp.where(west_b, from_west, jnp.where(east_b, from_east, loc[slot_b, f, rows, :]))
            state[f, pl.ds(64 * half, HALF, stride=8), :] = jnp.where(left, xa, xb)

    def pair(f, m):
        return state[f, pl.ds(m, HALF, stride=16), :], state[f, pl.ds(m + 8, HALF, stride=16), :]

    def mean(m):
        out = []
        for f in range(3):
            a, b = pair(f, m)
            out.append(0.5 * (a + b))
        return out

    def chain0(n, c):
        g = coarse(c, row)
        for f in range(3):
            ga[n, f] = g[f]
            state[f, pl.ds(n + 1, HALF, stride=16), :] = g[f]
            state[f, pl.ds(n + 9, HALF, stride=16), :] = g[f]
        return g

    lax.fori_loop(0, n_tm - 1, chain0, mean(0))

    fine(state, mid)

    def deliver(n, even, odd):
        for f in range(3):
            send[n, f, pl.ds(0, HALF, stride=2), :] = even[f]
            send[n, f, pl.ds(1, HALF, stride=2), :] = odd[f]

    def message(n):
        return pltpu.make_async_remote_copy(
            src_ref=send.at[n], dst_ref=recv.at[me], send_sem=tm_send.at[n], recv_sem=tm_recv.at[me],
            device_id=(n, own), device_id_type=MESH,
        )

    def dispatch(n):
        @pl.when(n != me)
        def _():
            message(n).start()

    pairs = [pair(f, 0) for f in range(3)]
    deliver(0, [a for a, _ in pairs], [b for _, b in pairs])
    dispatch(0)
    for f in range(3):
        delta[f, pl.ds(0, HALF, stride=8), :] = jnp.zeros((HALF, LANES), jnp.float32)

    def chain1(n, c):
        k = coarse(c, row)
        out = []
        for f in range(3):
            ka[n, f] = k[f]
            a, b = pair(f, n)
            d = k[f] - ga[n, f]
            delta[f, pl.ds(n, HALF, stride=8), :] = d
            out.append(d + 0.5 * (a + b))
        return out

    c = lax.fori_loop(1, n_tm - 1, chain1, mean(0))
    k = coarse(c, row)
    for f in range(3):
        ka[n_tm - 1, f] = k[f]
        delta[f, pl.ds(n_tm - 1, HALF, stride=8), :] = jnp.zeros((HALF, LANES), jnp.float32)
    for f in range(3):
        for j in range(HALF):
            d = delta[f, HALF * j : HALF * j + HALF, :]
            for i in (2 * j, 2 * j + 1):
                state[f, HALF * i : HALF * i + HALF, :] = state[f, HALF * i : HALF * i + HALF, :] + d

    fine(state, mid)
    pairs = [pair(f, 0) for f in range(3)]
    deliver(1, [a for a, _ in pairs], [b for _, b in pairs])
    dispatch(1)

    def chain2(n, c):
        k = coarse(c, row)
        even, odd, out = [], [], []
        for f in range(3):
            a, b = pair(f, n - 1)
            d = k[f] - ka[n, f]
            even.append(a + d)
            odd.append(b + d)
            out.append(d + 0.5 * (a + b))
        deliver(n, even, odd)
        dispatch(n)
        return out

    lax.fori_loop(2, n_tm, chain2, mean(0))

    recv[me] = send[me]
    for p in range(n_tm):
        @pl.when(p != me)
        def _():
            pltpu.make_async_remote_copy(
                src_ref=send.at[p], dst_ref=recv.at[p], send_sem=tm_send.at[p], recv_sem=tm_recv.at[p],
                device_id=(p, own), device_id_type=MESH,
            ).wait()

    for b in range(blocks):
        lo = LANES * b
        parts = [p for p in range(n_tm) if seg * p < lo + LANES and seg * p + seg > lo]
        for f in range(3):
            for half in range(2):
                rows = pl.ds(HALF * half, HALF)
                value = recv[parts[0], f, rows, :]
                for p in parts[1:]:
                    value = jnp.where(lane >= seg * p - lo, recv[p, f, rows, :], value)
                run[b, f, rows, :] = value
    for b in range(blocks):
        spot = jnp.int32(0)
        for i in range(1, blocks):
            spot = jnp.where(jnp.logical_and(order[i] == b, count > i), i, spot)
        out_ref[0, b] = jnp.where(lives[b], run[spot], 0.0)


def solution(mesh):
    n_tm, owners = mesh.shape["tm"], mesh.shape["space"]
    blocks = 3
    seg = blocks * LANES // n_tm

    def local(water_depth, momentum, slot_live, neighbours):
        f32 = jnp.float32
        dma = pltpu.SemaphoreType.DMA
        return pl.pallas_call(
            functools.partial(kernel, n_tm, owners, seg),
            out_shape=jax.ShapeDtypeStruct((1, blocks, 3, ROWS, LANES), f32),
            in_specs=[
                pl.BlockSpec(memory_space=pltpu.SMEM),
                pl.BlockSpec(memory_space=pltpu.SMEM),
                pl.BlockSpec(memory_space=pl.ANY),
                pl.BlockSpec(memory_space=pl.ANY),
            ],
            out_specs=pl.BlockSpec(memory_space=pltpu.VMEM),
            scratch_shapes=[
                pltpu.VMEM((blocks, 3, ROWS, LANES), f32),
                pltpu.VMEM((2, 3, ROWS, LANES), f32),
                pltpu.VMEM((2, 3, ROWS, LANES), f32),
                pltpu.VMEM((3, HALF * ROWS, LANES), f32),
                pltpu.VMEM((3, HALF * ROWS, LANES), f32),
                pltpu.VMEM((3, HALF * HALF, LANES), f32),
                pltpu.VMEM((n_tm, 3, HALF, LANES), f32),
                pltpu.VMEM((n_tm, 3, HALF, LANES), f32),
                pltpu.VMEM((n_tm, 3, ROWS, LANES), f32),
                pltpu.VMEM((n_tm, 3, ROWS, LANES), f32),
                pltpu.VMEM((blocks, 3, ROWS, LANES), f32),
                dma((2,)),
                dma((2,)),
                dma((2,)),
                dma((n_tm,)),
                dma((n_tm,)),
            ],
            compiler_params=pltpu.CompilerParams(collective_id=0, has_side_effects=True),
            name="parareal",
        )(slot_live, neighbours, water_depth, momentum)

    return jax.shard_map(
        local,
        mesh=mesh,
        in_specs=(P("space", None, None), P("space", None, None, None), P("space"), P("space", None)),
        out_specs=P("tm", "space", None, None, None),
        check_vma=False,
    )
```

```python
import functools

import jax
import jax.numpy as jnp
from jax import lax
from jax.experimental import pallas as pl
from jax.experimental.pallas import tpu as pltpu
from jax.sharding import PartitionSpec as P

SUB = 3
TIME_STEP = 0.15
ROWS = 16
HALF = 8
LANES = 128
MESH = pl.DeviceIdType.MESH


def pick(index, values):
    result = values[-1]
    for i in range(len(values) - 2, -1, -1):
        result = jnp.where(index == i, values[i], result)
    return result


def derived(h, m, n):
    r = lax.rsqrt(h)
    c = h * r
    inv = r * r
    u = m * inv
    q = n * inv
    p = 0.5 * h * h
    f1 = m * u + p
    f2 = n * u
    g2 = n * q + p
    sx = jnp.abs(u) + c
    sy = jnp.abs(q) + c
    return f1, f2, g2, sx, sy


def faces(a_v, b_v, a_f, b_f, a_s, b_s):
    top = jnp.maximum(a_s, b_s)
    return [(fa + fb) - top * (vb - va) for va, vb, fa, fb in zip(a_v, b_v, a_f, b_f)]


def shift(x, distance):
    return pltpu.roll(x, (-distance) % LANES, 1)


def rows_part(v, d, row):
    n = v[2]
    f1, f2, g2, sx, sy = d
    up = lambda x: pltpu.roll(x, HALF - 1, 0)
    down = lambda x: pltpu.roll(x, 1, 0)
    vn = [up(x) for x in v]
    wy = faces(v, vn, (n, f2, g2), (vn[2], up(f2), up(g2)), sy, up(sy))
    last, first = row == HALF - 1, row == 0
    sn = sy * n
    zero = jnp.zeros_like(n)
    high = [jnp.where(last, w, x) for w, x in zip((zero, zero, 2.0 * (g2 + sn)), wy)]
    low = [jnp.where(first, w, down(x)) for w, x in zip((zero, zero, 2.0 * (g2 - sn)), wy)]
    return [(-0.5 * TIME_STEP) * (x - y) for x, y in zip(high, low)]


def lane_face(v0, d0, v1, d1):
    return faces(v0, v1, (v0[1], d0[0], d0[1]), (v1[1], d1[0], d1[1]), d0[3], d1[3])


def coarse(v, row):
    a = -0.5 * TIME_STEP * SUB
    at = {o: [shift(x, o) if o else x for x in v] for o in (0, 1, -1, 2, -2)}
    d = {0: derived(*at[0])}
    across = {0: rows_part(at[0], d[0], row)}
    for o in (1, -1):
        across[o] = [shift(y, o) for y in across[0]]
    for o in (1, -1, 2, -2):
        d[o] = derived(*at[o])
    w = {o: lane_face(at[o], d[o], at[o + 1], d[o + 1]) for o in (0, -1, 1, -2)}
    v1 = {
        o: [x + (a * (r - l) + y) for x, r, l, y in zip(at[o], w[o], w[o - 1], across[o])]
        for o in (0, 1, -1)
    }
    e = {o: derived(*v1[o]) for o in (0, 1, -1)}
    across1 = rows_part(v1[0], e[0], row)
    w1 = {o: lane_face(v1[o], e[o], v1[o + 1], e[o + 1]) for o in (0, -1)}
    return [
        0.5 * ((x + x1) + (a * (r - l) + y))
        for x, x1, r, l, y in zip(v, v1[0], w1[0], w1[-1], across1)
    ]


def fine_pass(load, emit, ahead=2):
    v, d, e, w = {}, {}, {}, {}
    low = None
    for t in range(ROWS + 2 * ahead):
        if t < ROWS:
            v[t] = load(t)
            d[t] = derived(*v[t])
            e[t] = [shift(x, 1) for x in (*v[t], d[t][0], d[t][1], d[t][3])]
        j = t - ahead
        if 0 <= j < ROWS:
            f1, f2, g2, sx, sy = d[j]
            x = e[j]
            wx = faces(v[j], x[:3], (v[j][1], f1, f2), (x[1], x[3], x[4]), sx, x[5])
            w[j] = (wx, [shift(y, -1) for y in wx])
        j = t - 2 * ahead
        if 0 <= j < ROWS:
            h, m, n = v[j]
            f1, f2, g2, sx, sy = d[j]
            if j == 0:
                low = [None, None, 2.0 * (g2 - sy * n)]
            if j + 1 < ROWS:
                f1a, f2a, g2a, sxa, sya = d[j + 1]
                high = faces(v[j], v[j + 1], (n, f2, g2), (v[j + 1][2], f2a, g2a), sy, sya)
            else:
                high = [None, None, 2.0 * (g2 + sy * n)]
            diff = []
            for right, left, hi, lo in zip(*w[j], high, low):
                y = right - left
                if hi is not None:
                    y = y + hi
                if lo is not None:
                    y = y - lo
                diff.append(y)
            emit(j, v[j], diff)
            low = high


def fine(state, mid):
    def at(ref, j):
        return [ref[f, HALF * j : HALF * j + HALF, :] for f in range(3)]

    def put(ref, j, v):
        for f in range(3):
            ref[f, HALF * j : HALF * j + HALF, :] = v[f]

    def first(j, v, d):
        put(mid, j, [x - (0.5 * TIME_STEP) * y for x, y in zip(v, d)])

    def second(j, v1, d):
        v = at(state, j)
        put(state, j, [0.5 * (x + y) - (0.25 * TIME_STEP) * z for x, y, z in zip(v, v1, d)])

    def once(i, run):
        def trip(_, carry):
            run()
            return carry

        lax.fori_loop(0, jnp.minimum(i, 0) + 1, trip, 0)

    def step(i, carry):
        once(i, lambda: fine_pass(lambda j: at(state, j), first))
        once(i, lambda: fine_pass(lambda j: at(mid, j), second))
        return carry

    lax.fori_loop(0, SUB, step, 0)


def kernel(
    n_tm, owners, seg,
    live_ref, nb_ref, depth_ref, mom_ref, out_ref,
    loc, edge, got, state, mid, delta, ga, ka, send, recv, run,
    in_sem, edge_send, edge_recv, tm_send, tm_recv,
):
    me = lax.axis_index("tm")
    own = lax.axis_index("space")
    east_owner = lax.rem(own + 1, owners)
    west_owner = lax.rem(own + owners - 1, owners)
    blocks = loc.shape[0]

    in_copies = [
        pltpu.make_async_copy(depth_ref, loc.at[:, 0], in_sem.at[0]),
        pltpu.make_async_copy(mom_ref, loc.at[:, 1:3], in_sem.at[1]),
    ]
    for c in in_copies:
        c.start()

    barrier = pltpu.get_barrier_semaphore()
    for o in (west_owner, east_owner):
        pl.semaphore_signal(barrier, inc=1, device_id=(me, o), device_id_type=MESH)
    for d in range(1, n_tm):
        peer = lax.rem(me + d, n_tm)
        pl.semaphore_signal(barrier, inc=1, device_id=(peer, own), device_id_type=MESH)

    lives = [live_ref[b] == 1 for b in range(blocks)]
    wests = [nb_ref[0, b] for b in range(blocks)]
    easts = [nb_ref[1, b] for b in range(blocks)]
    count = jnp.int32(0)
    first = jnp.int32(0)
    final = jnp.int32(0)
    for b in range(blocks):
        count = count + jnp.where(lives[b], 1, 0)
        first = first + jnp.where(jnp.logical_and(lives[b], wests[b] == blocks), b, 0)
        final = final + jnp.where(jnp.logical_and(lives[b], easts[b] == blocks), b, 0)
    order = [first]
    for _ in range(blocks - 1):
        order.append(jnp.minimum(pick(order[-1], easts), blocks - 1))

    for c in in_copies:
        c.wait()
    edge[0] = loc[first]
    edge[1] = loc[final]
    pl.semaphore_wait(barrier, n_tm + 1)
    halo = [
        pltpu.make_async_remote_copy(
            src_ref=edge.at[i], dst_ref=got.at[i], send_sem=edge_send.at[i], recv_sem=edge_recv.at[i],
            device_id=(me, o), device_id_type=MESH,
        )
        for i, o in ((0, west_owner), (1, east_owner))
    ]
    for c in halo:
        c.start()

    pad = (LANES - seg) // 2
    begin = seg * me + (LANES - pad)
    place = begin // LANES - 1
    offset = begin % LANES
    lane = lax.broadcasted_iota(jnp.int32, (HALF, LANES), 1)
    row = lax.broadcasted_iota(jnp.int32, (HALF, LANES), 0)
    left = lane >= offset

    for c in halo:
        c.wait()

    def source(position):
        slot = pick(position, order)
        return slot, position < 0, position >= count

    slot_a, west_a, east_a = source(place)
    slot_b, west_b, east_b = source(place + 1)
    slot_a = jnp.clip(slot_a, 0, blocks - 1)
    slot_b = jnp.clip(slot_b, 0, blocks - 1)
    for f in range(3):
        for half in range(2):
            rows = pl.ds(HALF * half, HALF)
            from_east, from_west = got[0, f, rows, :], got[1, f, rows, :]
            xa = jnp.where(west_a, from_west, jnp.where(east_a, from_east, loc[slot_a, f, rows, :]))
            xb = jnp.where(west_b, from_west, jnp.where(east_b, from_east, loc[slot_b, f, rows, :]))
            state[f, pl.ds(64 * half, HALF, stride=8), :] = jnp.where(left, xa, xb)

    def pair(f, m):
        return state[f, pl.ds(m, HALF, stride=16), :], state[f, pl.ds(m + 8, HALF, stride=16), :]

    def mean(m):
        out = []
        for f in range(3):
            a, b = pair(f, m)
            out.append(0.5 * (a + b))
        return out

    def chain0(n, c):
        g = coarse(c, row)
        for f in range(3):
            ga[n, f] = g[f]
            state[f, pl.ds(n + 1, HALF, stride=16), :] = g[f]
            state[f, pl.ds(n + 9, HALF, stride=16), :] = g[f]
        return g

    lax.fori_loop(0, n_tm - 1, chain0, mean(0))

    fine(state, mid)

    def deliver(n, even, odd):
        for f in range(3):
            send[n, f, pl.ds(0, HALF, stride=2), :] = even[f]
            send[n, f, pl.ds(1, HALF, stride=2), :] = odd[f]

    def message(n):
        return pltpu.make_async_remote_copy(
            src_ref=send.at[n], dst_ref=recv.at[me], send_sem=tm_send.at[n], recv_sem=tm_recv.at[me],
            device_id=(n, own), device_id_type=MESH,
        )

    def dispatch(n):
        @pl.when(n != me)
        def _():
            message(n).start()

    pairs = [pair(f, 0) for f in range(3)]
    deliver(0, [a for a, _ in pairs], [b for _, b in pairs])
    dispatch(0)
    for f in range(3):
        delta[f, pl.ds(0, HALF, stride=8), :] = jnp.zeros((HALF, LANES), jnp.float32)

    def chain1(n, c):
        k = coarse(c, row)
        out = []
        for f in range(3):
            ka[n, f] = k[f]
            a, b = pair(f, n)
            d = k[f] - ga[n, f]
            delta[f, pl.ds(n, HALF, stride=8), :] = d
            out.append(d + 0.5 * (a + b))
        return out

    c = lax.fori_loop(1, n_tm - 1, chain1, mean(0))
    k = coarse(c, row)
    for f in range(3):
        ka[n_tm - 1, f] = k[f]
        delta[f, pl.ds(n_tm - 1, HALF, stride=8), :] = jnp.zeros((HALF, LANES), jnp.float32)
    for f in range(3):
        for j in range(HALF):
            d = delta[f, HALF * j : HALF * j + HALF, :]
            for i in (2 * j, 2 * j + 1):
                state[f, HALF * i : HALF * i + HALF, :] = state[f, HALF * i : HALF * i + HALF, :] + d

    fine(state, mid)
    pairs = [pair(f, 0) for f in range(3)]
    deliver(1, [a for a, _ in pairs], [b for _, b in pairs])
    dispatch(1)

    def chain2(n, c):
        k = coarse(c, row)
        even, odd, out = [], [], []
        for f in range(3):
            a, b = pair(f, n - 1)
            d = k[f] - ka[n, f]
            even.append(a + d)
            odd.append(b + d)
            out.append(d + 0.5 * (a + b))
        deliver(n, even, odd)
        dispatch(n)
        return out

    lax.fori_loop(2, n_tm, chain2, mean(0))

    recv[me] = send[me]
    for p in range(n_tm):
        @pl.when(p != me)
        def _():
            pltpu.make_async_remote_copy(
                src_ref=send.at[p], dst_ref=recv.at[p], send_sem=tm_send.at[p], recv_sem=tm_recv.at[p],
                device_id=(p, own), device_id_type=MESH,
            ).wait()

    for b in range(blocks):
        lo = LANES * b
        parts = [p for p in range(n_tm) if seg * p < lo + LANES and seg * p + seg > lo]
        for f in range(3):
            for half in range(2):
                rows = pl.ds(HALF * half, HALF)
                value = recv[parts[0], f, rows, :]
                for p in parts[1:]:
                    value = jnp.where(lane >= seg * p - lo, recv[p, f, rows, :], value)
                run[b, f, rows, :] = value
    for b in range(blocks):
        spot = jnp.int32(0)
        for i in range(1, blocks):
            spot = jnp.where(jnp.logical_and(order[i] == b, count > i), i, spot)
        out_ref[0, b] = jnp.where(lives[b], run[spot], 0.0)


def solution(mesh):
    n_tm, owners = mesh.shape["tm"], mesh.shape["space"]
    blocks = 3
    seg = blocks * LANES // n_tm

    def local(water_depth, momentum, slot_live, neighbours):
        f32 = jnp.float32
        dma = pltpu.SemaphoreType.DMA
        return pl.pallas_call(
            functools.partial(kernel, n_tm, owners, seg),
            out_shape=jax.ShapeDtypeStruct((1, blocks, 3, ROWS, LANES), f32),
            in_specs=[
                pl.BlockSpec(memory_space=pltpu.SMEM),
                pl.BlockSpec(memory_space=pltpu.SMEM),
                pl.BlockSpec(memory_space=pl.ANY),
                pl.BlockSpec(memory_space=pl.ANY),
            ],
            out_specs=pl.BlockSpec(memory_space=pltpu.VMEM),
            scratch_shapes=[
                pltpu.VMEM((blocks, 3, ROWS, LANES), f32),
                pltpu.VMEM((2, 3, ROWS, LANES), f32),
                pltpu.VMEM((2, 3, ROWS, LANES), f32),
                pltpu.VMEM((3, HALF * ROWS, LANES), f32),
                pltpu.VMEM((3, HALF * ROWS, LANES), f32),
                pltpu.VMEM((3, HALF * HALF, LANES), f32),
                pltpu.VMEM((n_tm, 3, HALF, LANES), f32),
                pltpu.VMEM((n_tm, 3, HALF, LANES), f32),
                pltpu.VMEM((n_tm, 3, ROWS, LANES), f32),
                pltpu.VMEM((n_tm, 3, ROWS, LANES), f32),
                pltpu.VMEM((blocks, 3, ROWS, LANES), f32),
                dma((2,)),
                dma((2,)),
                dma((2,)),
                dma((n_tm,)),
                dma((n_tm,)),
            ],
            compiler_params=pltpu.CompilerParams(collective_id=0, has_side_effects=True),
            name="parareal",
        )(slot_live, neighbours.T, water_depth, momentum)

    return jax.shard_map(
        local,
        mesh=mesh,
        in_specs=(P("space", None, None), P("space", None, None, None), P("space"), P("space", None)),
        out_specs=P("tm", "space", None, None, None),
        check_vma=False,
    )
```

```python
import functools

import jax
import jax.numpy as jnp
from jax import lax
from jax.experimental import pallas as pl
from jax.experimental.pallas import tpu as pltpu
from jax.sharding import PartitionSpec as P

SUB = 3
TIME_STEP = 0.15
ROWS = 16
HALF = 8
LANES = 128
SLICES_REACH = 24
VMEM_LIMIT = 60 * 1024 * 1024
MESH = pl.DeviceIdType.MESH


def pick(index, values):
    result = values[-1]
    for i in range(len(values) - 2, -1, -1):
        result = jnp.where(index == i, values[i], result)
    return result


def derived(h, m, n):
    r = lax.rsqrt(h)
    c = h * r
    inv = r * r
    u = m * inv
    q = n * inv
    p = 0.5 * h * h
    f1 = m * u + p
    f2 = n * u
    g2 = n * q + p
    sx = jnp.abs(u) + c
    sy = jnp.abs(q) + c
    return f1, f2, g2, sx, sy


def faces(a_v, b_v, a_f, b_f, a_s, b_s):
    top = jnp.maximum(a_s, b_s)
    return [(fa + fb) - top * (vb - va) for va, vb, fa, fb in zip(a_v, b_v, a_f, b_f)]


def shift(x, distance):
    return pltpu.roll(x, (-distance) % LANES, 1)


def rows_part(v, d, row):
    n = v[2]
    f1, f2, g2, sx, sy = d
    up = lambda x: pltpu.roll(x, HALF - 1, 0)
    down = lambda x: pltpu.roll(x, 1, 0)
    vn = [up(x) for x in v]
    wy = faces(v, vn, (n, f2, g2), (vn[2], up(f2), up(g2)), sy, up(sy))
    last, first = row == HALF - 1, row == 0
    sn = sy * n
    zero = jnp.zeros_like(n)
    high = [jnp.where(last, w, x) for w, x in zip((zero, zero, 2.0 * (g2 + sn)), wy)]
    low = [jnp.where(first, w, down(x)) for w, x in zip((zero, zero, 2.0 * (g2 - sn)), wy)]
    return [(-0.5 * TIME_STEP) * (x - y) for x, y in zip(high, low)]


def lane_face(v0, d0, v1, d1):
    return faces(v0, v1, (v0[1], d0[0], d0[1]), (v1[1], d1[0], d1[1]), d0[3], d1[3])


def coarse(v, row):
    a = -0.5 * TIME_STEP * SUB
    at = {o: [shift(x, o) if o else x for x in v] for o in (0, 1, -1, 2, -2)}
    d = {0: derived(*at[0])}
    across = {0: rows_part(at[0], d[0], row)}
    for o in (1, -1):
        across[o] = [shift(y, o) for y in across[0]]
    for o in (1, -1, 2, -2):
        d[o] = derived(*at[o])
    w = {o: lane_face(at[o], d[o], at[o + 1], d[o + 1]) for o in (0, -1, 1, -2)}
    v1 = {
        o: [x + (a * (r - l) + y) for x, r, l, y in zip(at[o], w[o], w[o - 1], across[o])]
        for o in (0, 1, -1)
    }
    e = {o: derived(*v1[o]) for o in (0, 1, -1)}
    across1 = rows_part(v1[0], e[0], row)
    w1 = {o: lane_face(v1[o], e[o], v1[o + 1], e[o + 1]) for o in (0, -1)}
    return [
        0.5 * ((x + x1) + (a * (r - l) + y))
        for x, x1, r, l, y in zip(v, v1[0], w1[0], w1[-1], across1)
    ]


def fine_pass(load, emit, ahead=2):
    v, d, e, w = {}, {}, {}, {}
    low = None
    for t in range(ROWS + 2 * ahead):
        if t < ROWS:
            v[t] = load(t)
            d[t] = derived(*v[t])
            e[t] = [shift(x, 1) for x in (*v[t], d[t][0], d[t][1], d[t][3])]
        j = t - ahead
        if 0 <= j < ROWS:
            f1, f2, g2, sx, sy = d[j]
            x = e[j]
            wx = faces(v[j], x[:3], (v[j][1], f1, f2), (x[1], x[3], x[4]), sx, x[5])
            w[j] = (wx, [shift(y, -1) for y in wx])
        j = t - 2 * ahead
        if 0 <= j < ROWS:
            h, m, n = v[j]
            f1, f2, g2, sx, sy = d[j]
            if j == 0:
                low = [None, None, 2.0 * (g2 - sy * n)]
            if j + 1 < ROWS:
                f1a, f2a, g2a, sxa, sya = d[j + 1]
                high = faces(v[j], v[j + 1], (n, f2, g2), (v[j + 1][2], f2a, g2a), sy, sya)
            else:
                high = [None, None, 2.0 * (g2 + sy * n)]
            diff = []
            for right, left, hi, lo in zip(*w[j], high, low):
                y = right - left
                if hi is not None:
                    y = y + hi
                if lo is not None:
                    y = y - lo
                diff.append(y)
            emit(j, v[j], diff)
            low = high


def fine(state, mid):
    def at(ref, j):
        return [ref[f, HALF * j : HALF * j + HALF, :] for f in range(3)]

    def put(ref, j, v):
        for f in range(3):
            ref[f, HALF * j : HALF * j + HALF, :] = v[f]

    def first(j, v, d):
        put(mid, j, [x - (0.5 * TIME_STEP) * y for x, y in zip(v, d)])

    def second(j, v1, d):
        v = at(state, j)
        put(state, j, [0.5 * (x + y) - (0.25 * TIME_STEP) * z for x, y, z in zip(v, v1, d)])

    def once(i, run):
        def trip(_, carry):
            run()
            return carry

        lax.fori_loop(0, jnp.minimum(i, 0) + 1, trip, 0)

    def step(i, carry):
        once(i, lambda: fine_pass(lambda j: at(state, j), first))
        once(i, lambda: fine_pass(lambda j: at(mid, j), second))
        return carry

    lax.fori_loop(0, SUB, step, 0)


def seams(n_tm, blocks, seg):
    reach = SLICES_REACH
    west = [n for n in range(n_tm) if seg * n - reach < 0]
    east = [
        n
        for n in range(n_tm)
        if any(seg * n < LANES * k < seg * n + seg + reach for k in range(1, blocks + 1))
    ]
    assert not set(west) & set(east)
    return west, east


def member(me, places):
    return functools.reduce(jnp.logical_or, [me == n for n in places])


def tables(live_ref, nb_ref, blocks):
    lives = [live_ref[b] == 1 for b in range(blocks)]
    count = jnp.int32(0)
    first = jnp.int32(0)
    final = jnp.int32(0)
    for b in range(blocks):
        count = count + jnp.where(lives[b], 1, 0)
        first = first + jnp.where(jnp.logical_and(lives[b], nb_ref[0, b] == blocks), b, 0)
        final = final + jnp.where(jnp.logical_and(lives[b], nb_ref[1, b] == blocks), b, 0)
    easts = [nb_ref[1, b] for b in range(blocks)]
    order = [first]
    for _ in range(blocks - 1):
        order.append(jnp.minimum(pick(order[-1], easts), blocks - 1))
    return lives, count, final, order


def window_kernel(
    n_tm, owners, seg,
    live_hbm, nb_hbm, depth_ref, mom_ref, win_ref,
    loc, edge, got, live_ref, nb_ref,
    in_sem, edge_send, edge_recv,
):
    me = lax.axis_index("tm")
    own = lax.axis_index("space")
    east_owner = lax.rem(own + 1, owners)
    west_owner = lax.rem(own + owners - 1, owners)
    blocks = loc.shape[0]
    west_set, east_set = seams(n_tm, blocks, seg)
    at_west, at_east = member(me, west_set), member(me, east_set)
    at_seam = jnp.logical_or(at_west, at_east)

    copies = [
        pltpu.make_async_copy(nb_hbm, nb_ref, in_sem.at[0]),
        pltpu.make_async_copy(live_hbm, live_ref, in_sem.at[1]),
        pltpu.make_async_copy(depth_ref, loc.at[:, 0], in_sem.at[2]),
        pltpu.make_async_copy(mom_ref, loc.at[:, 1:3], in_sem.at[3]),
    ]
    for c in copies:
        c.start()
    barrier = pltpu.get_barrier_semaphore()

    @pl.when(at_seam)
    def _():
        for o in (west_owner, east_owner):
            pl.semaphore_signal(barrier, inc=1, device_id=(me, o), device_id_type=MESH)

    for c in copies:
        c.wait()
    lives, count, final, order = tables(live_ref, nb_ref, blocks)

    halo = pltpu.make_async_remote_copy(
        src_ref=edge, dst_ref=got, send_sem=edge_send, recv_sem=edge_recv,
        device_id=(me, jnp.where(at_west, east_owner, west_owner)), device_id_type=MESH,
    )
    edge[...] = loc[jnp.where(at_west, final, order[0])]

    @pl.when(at_seam)
    def _():
        pl.semaphore_wait(barrier, 2)
        halo.start()

    pad = (LANES - seg) // 2
    begin = seg * me + (LANES - pad)
    place = begin // LANES - 1
    offset = begin % LANES
    lane = lax.broadcasted_iota(jnp.int32, (3, ROWS, LANES), 2)
    left = lane >= offset

    def slot(position):
        return jnp.clip(pick(position, order), 0, blocks - 1)

    win_ref[...] = jnp.where(left, loc[slot(place)], loc[slot(place + 1)])

    @pl.when(at_seam)
    def _():
        halo.wait()
        outside_a = jnp.logical_or(place < 0, place >= count)
        outside_b = place + 1 >= count
        mask = jnp.logical_or(
            jnp.logical_and(left, outside_a), jnp.logical_and(jnp.logical_not(left), outside_b)
        )
        win_ref[...] = jnp.where(mask, got[...], win_ref[...])


def main_kernel(
    n_tm, seg,
    live_hbm, nb_hbm, win_ref, out_ref,
    state, mid, delta, ga, ka, send, recv, run, live_ref, nb_ref,
    in_sem, tm_send, tm_recv,
):
    me = lax.axis_index("tm")
    own = lax.axis_index("space")
    blocks = out_ref.shape[1]
    copies = [
        pltpu.make_async_copy(nb_hbm, nb_ref, in_sem.at[0]),
        pltpu.make_async_copy(live_hbm, live_ref, in_sem.at[1]),
    ]
    for c in copies:
        c.start()
    barrier = pltpu.get_barrier_semaphore()
    for d in range(1, n_tm):
        peer = lax.rem(me + d, n_tm)
        pl.semaphore_signal(barrier, inc=1, device_id=(peer, own), device_id_type=MESH)

    row = lax.broadcasted_iota(jnp.int32, (HALF, LANES), 0)
    for f in range(3):
        for half in range(2):
            rows = win_ref[f, pl.ds(HALF * half, HALF), :]
            for m in (0, n_tm - 1):
                state[f, pl.ds(64 * half + m, HALF, stride=8), :] = rows

    def pair(f, m):
        return state[f, pl.ds(m, HALF, stride=16), :], state[f, pl.ds(m + 8, HALF, stride=16), :]

    def mean(m):
        out = []
        for f in range(3):
            a, b = pair(f, m)
            out.append(0.5 * (a + b))
        return out

    def chain0(n, c):
        g = coarse(c, row)
        for f in range(3):
            ga[n, f] = g[f]
            state[f, pl.ds(n + 1, HALF, stride=16), :] = g[f]
            state[f, pl.ds(n + 9, HALF, stride=16), :] = g[f]
        return g

    c6 = lax.fori_loop(0, n_tm - 2, chain0, mean(0))

    fine(state, mid)

    def deliver(n, even, odd):
        for f in range(3):
            send[n, f, pl.ds(0, HALF, stride=2), :] = even[f]
            send[n, f, pl.ds(1, HALF, stride=2), :] = odd[f]

    def message(n):
        return pltpu.make_async_remote_copy(
            src_ref=send.at[n], dst_ref=recv.at[me], send_sem=tm_send.at[n], recv_sem=tm_recv.at[me],
            device_id=(n, own), device_id_type=MESH,
        )

    def dispatch(n):
        @pl.when(n != me)
        def _():
            message(n).start()

    pairs = [pair(f, 0) for f in range(3)]
    deliver(0, [a for a, _ in pairs], [b for _, b in pairs])
    pl.semaphore_wait(barrier, n_tm - 1)
    dispatch(0)
    for f in range(3):
        for m in (0, n_tm - 1):
            delta[f, pl.ds(m, HALF, stride=8), :] = jnp.zeros((HALF, LANES), jnp.float32)

    def keep1(n, k, g):
        out = []
        for f in range(3):
            ka[n, f] = k[f]
            a, b = pair(f, n)
            d = k[f] - g[f]
            delta[f, pl.ds(n, HALF, stride=8), :] = d
            out.append(d + 0.5 * (a + b))
        return out

    k1, g6 = coarse(mean(0), row), coarse(c6, row)
    for f in range(3):
        ga[n_tm - 2, f] = g6[f]
    c = keep1(1, k1, [ga[1, f] for f in range(3)])

    def chain1(n, c):
        return keep1(n, coarse(c, row), [ga[n, f] for f in range(3)])

    c7 = lax.fori_loop(2, n_tm - 1, chain1, c)
    for f in range(3):
        for j in range(HALF):
            d = delta[f, HALF * j : HALF * j + HALF, :]
            for i in (2 * j, 2 * j + 1):
                state[f, HALF * i : HALF * i + HALF, :] = state[f, HALF * i : HALF * i + HALF, :] + d

    fine(state, mid)
    pairs = [pair(f, 0) for f in range(3)]
    deliver(1, [a for a, _ in pairs], [b for _, b in pairs])
    dispatch(1)

    def keep2(n, k):
        even, odd, out = [], [], []
        for f in range(3):
            a, b = pair(f, n - 1)
            d = k[f] - ka[n, f]
            even.append(a + d)
            odd.append(b + d)
            out.append(d + 0.5 * (a + b))
        deliver(n, even, odd)
        dispatch(n)
        return out

    k2, k7 = coarse(mean(0), row), coarse(c7, row)
    for f in range(3):
        ka[n_tm - 1, f] = k7[f]
    lax.fori_loop(3, n_tm, lambda n, c: keep2(n, coarse(c, row)), keep2(2, k2))

    recv[me] = send[me]
    for c in copies:
        c.wait()
    lives, count, _, order = tables(live_ref, nb_ref, blocks)
    for p in range(n_tm):
        @pl.when(p != me)
        def _():
            pltpu.make_async_remote_copy(
                src_ref=send.at[p], dst_ref=recv.at[p], send_sem=tm_send.at[p], recv_sem=tm_recv.at[p],
                device_id=(p, own), device_id_type=MESH,
            ).wait()

    lane = lax.broadcasted_iota(jnp.int32, (HALF, LANES), 1)
    for b in range(blocks):
        lo = LANES * b
        parts = [p for p in range(n_tm) if seg * p < lo + LANES and seg * p + seg > lo]
        for f in range(3):
            for half in range(2):
                rows = pl.ds(HALF * half, HALF)
                value = recv[parts[0], f, rows, :]
                for p in parts[1:]:
                    value = jnp.where(lane >= seg * p - lo, recv[p, f, rows, :], value)
                run[b, f, rows, :] = value
    for b in range(blocks):
        spot = jnp.int32(0)
        for i in range(1, blocks):
            spot = jnp.where(jnp.logical_and(order[i] == b, count > i), i, spot)
        out_ref[0, b] = jnp.where(lives[b], run[spot], 0.0)


def solution(mesh):
    n_tm, owners = mesh.shape["tm"], mesh.shape["space"]
    blocks = 3
    seg = blocks * LANES // n_tm
    f32, i32 = jnp.float32, jnp.int32
    dma = pltpu.SemaphoreType.DMA
    hbm = pl.BlockSpec(memory_space=pltpu.HBM)
    vmem = pl.BlockSpec(memory_space=pltpu.VMEM)
    small = [pltpu.SMEM((blocks,), i32), pltpu.SMEM((2, blocks), i32)]

    def local(water_depth, momentum, slot_live, neighbours):
        sides = neighbours.T
        window = pl.pallas_call(
            functools.partial(window_kernel, n_tm, owners, seg),
            out_shape=pltpu.VMEM((3, ROWS, LANES), f32),
            in_specs=[hbm] * 4,
            out_specs=vmem,
            scratch_shapes=[
                pltpu.VMEM((blocks, 3, ROWS, LANES), f32),
                pltpu.VMEM((3, ROWS, LANES), f32),
                pltpu.VMEM((3, ROWS, LANES), f32),
                *small,
                dma((4,)),
                dma,
                dma,
            ],
            compiler_params=pltpu.CompilerParams(collective_id=0, has_side_effects=True, vmem_limit_bytes=VMEM_LIMIT),
            name="window",
        )(slot_live, sides, water_depth, momentum)
        return pl.pallas_call(
            functools.partial(main_kernel, n_tm, seg),
            out_shape=pltpu.VMEM((1, blocks, 3, ROWS, LANES), f32),
            in_specs=[hbm, hbm, vmem],
            out_specs=vmem,
            scratch_shapes=[
                pltpu.VMEM((3, HALF * ROWS, LANES), f32),
                pltpu.VMEM((3, HALF * ROWS, LANES), f32),
                pltpu.VMEM((3, HALF * HALF, LANES), f32),
                pltpu.VMEM((n_tm, 3, HALF, LANES), f32),
                pltpu.VMEM((n_tm, 3, HALF, LANES), f32),
                pltpu.VMEM((n_tm, 3, ROWS, LANES), f32),
                pltpu.VMEM((n_tm, 3, ROWS, LANES), f32),
                pltpu.VMEM((blocks, 3, ROWS, LANES), f32),
                *small,
                dma((2,)),
                dma((n_tm,)),
                dma((n_tm,)),
            ],
            compiler_params=pltpu.CompilerParams(collective_id=1, has_side_effects=True, vmem_limit_bytes=VMEM_LIMIT),
            name="parareal",
        )(slot_live, sides, pltpu.with_memory_space_constraint(window, pltpu.VMEM))

    return jax.shard_map(
        local,
        mesh=mesh,
        in_specs=(P("space", None, None), P("space", None, None, None), P("space"), P("space", None)),
        out_specs=P("tm", "space", None, None, None),
        check_vma=False,
    )
```

```python
import functools

import jax
import jax.numpy as jnp
from jax import lax
from jax.experimental import pallas as pl
from jax.experimental.pallas import tpu as pltpu
from jax.sharding import PartitionSpec as P

SUB = 3
TIME_STEP = 0.15
ROWS = 16
HALF = 8
LANES = 128
REACH = 24
STARTS = (0, 48, 96, 144, 192, 232, 288, 336, 384)
HOLDS = (1, 0, 3, 2, 4, 7, 6, 5)
VMEM_LIMIT = 60 * 1024 * 1024
MESH = pl.DeviceIdType.MESH


def pick(index, values):
    result = values[-1]
    for i in range(len(values) - 2, -1, -1):
        result = jnp.where(index == i, values[i], result)
    return result


def derived(h, m, n):
    r = lax.rsqrt(h)
    c = h * r
    inv = r * r
    u = m * inv
    q = n * inv
    p = 0.5 * h * h
    f1 = m * u + p
    f2 = n * u
    g2 = n * q + p
    sx = jnp.abs(u) + c
    sy = jnp.abs(q) + c
    return f1, f2, g2, sx, sy


def faces(a_v, b_v, a_f, b_f, a_s, b_s):
    top = jnp.maximum(a_s, b_s)
    return [(fa + fb) - top * (vb - va) for va, vb, fa, fb in zip(a_v, b_v, a_f, b_f)]


def shift(x, distance):
    return pltpu.roll(x, (-distance) % LANES, 1)


def rows_part(v, d, row):
    n = v[2]
    f1, f2, g2, sx, sy = d
    up = lambda x: pltpu.roll(x, HALF - 1, 0)
    down = lambda x: pltpu.roll(x, 1, 0)
    vn = [up(x) for x in v]
    wy = faces(v, vn, (n, f2, g2), (vn[2], up(f2), up(g2)), sy, up(sy))
    last, first = row == HALF - 1, row == 0
    sn = sy * n
    zero = jnp.zeros_like(n)
    high = [jnp.where(last, w, x) for w, x in zip((zero, zero, 2.0 * (g2 + sn)), wy)]
    low = [jnp.where(first, w, down(x)) for w, x in zip((zero, zero, 2.0 * (g2 - sn)), wy)]
    return [(-0.5 * TIME_STEP) * (x - y) for x, y in zip(high, low)]


def lane_face(v0, d0, v1, d1):
    return faces(v0, v1, (v0[1], d0[0], d0[1]), (v1[1], d1[0], d1[1]), d0[3], d1[3])


def coarse(v, row):
    a = -0.5 * TIME_STEP * SUB
    at = {o: [shift(x, o) if o else x for x in v] for o in (0, 1, -1, 2, -2)}
    d = {0: derived(*at[0])}
    across = {0: rows_part(at[0], d[0], row)}
    for o in (1, -1):
        across[o] = [shift(y, o) for y in across[0]]
    for o in (1, -1, 2, -2):
        d[o] = derived(*at[o])
    w = {o: lane_face(at[o], d[o], at[o + 1], d[o + 1]) for o in (0, -1, 1, -2)}
    v1 = {
        o: [x + (a * (r - l) + y) for x, r, l, y in zip(at[o], w[o], w[o - 1], across[o])]
        for o in (0, 1, -1)
    }
    e = {o: derived(*v1[o]) for o in (0, 1, -1)}
    across1 = rows_part(v1[0], e[0], row)
    w1 = {o: lane_face(v1[o], e[o], v1[o + 1], e[o + 1]) for o in (0, -1)}
    return [
        0.5 * ((x + x1) + (a * (r - l) + y))
        for x, x1, r, l, y in zip(v, v1[0], w1[0], w1[-1], across1)
    ]


def fine_pass(load, emit, ahead=2):
    v, d, e, w = {}, {}, {}, {}
    low = None
    for t in range(ROWS + 2 * ahead):
        if t < ROWS:
            v[t] = load(t)
            d[t] = derived(*v[t])
            e[t] = [shift(x, 1) for x in (*v[t], d[t][0], d[t][1], d[t][3])]
        j = t - ahead
        if 0 <= j < ROWS:
            f1, f2, g2, sx, sy = d[j]
            x = e[j]
            wx = faces(v[j], x[:3], (v[j][1], f1, f2), (x[1], x[3], x[4]), sx, x[5])
            w[j] = (wx, [shift(y, -1) for y in wx])
        j = t - 2 * ahead
        if 0 <= j < ROWS:
            h, m, n = v[j]
            f1, f2, g2, sx, sy = d[j]
            if j == 0:
                low = [None, None, 2.0 * (g2 - sy * n)]
            if j + 1 < ROWS:
                f1a, f2a, g2a, sxa, sya = d[j + 1]
                high = faces(v[j], v[j + 1], (n, f2, g2), (v[j + 1][2], f2a, g2a), sy, sya)
            else:
                high = [None, None, 2.0 * (g2 + sy * n)]
            diff = []
            for right, left, hi, lo in zip(*w[j], high, low):
                y = right - left
                if hi is not None:
                    y = y + hi
                if lo is not None:
                    y = y - lo
                diff.append(y)
            emit(j, v[j], diff)
            low = high


def fine(state, mid):
    def at(ref, j):
        return [ref[f, HALF * j : HALF * j + HALF, :] for f in range(3)]

    def put(ref, j, v):
        for f in range(3):
            ref[f, HALF * j : HALF * j + HALF, :] = v[f]

    def first(j, v, d):
        put(mid, j, [x - (0.5 * TIME_STEP) * y for x, y in zip(v, d)])

    def second(j, v1, d):
        v = at(state, j)
        put(state, j, [0.5 * (x + y) - (0.25 * TIME_STEP) * z for x, y, z in zip(v, v1, d)])

    def once(i, run):
        def trip(_, carry):
            run()
            return carry

        lax.fori_loop(0, jnp.minimum(i, 0) + 1, trip, 0)

    def step(i, carry):
        once(i, lambda: fine_pass(lambda j: at(state, j), first))
        once(i, lambda: fine_pass(lambda j: at(mid, j), second))
        return carry

    lax.fori_loop(0, SUB, step, 0)


def seams(blocks):
    spans = [(STARTS[k], STARTS[k + 1]) for k in HOLDS]
    west = [n for n, (lo, _) in enumerate(spans) if lo < REACH]
    east = [
        n
        for n, (lo, hi) in enumerate(spans)
        if any(lo < LANES * k < hi + REACH for k in range(1, blocks + 1))
    ]
    assert not set(west) & set(east)
    assert max(hi - lo for lo, hi in spans) + 2 * REACH <= LANES
    return west, east


def member(me, places):
    return functools.reduce(jnp.logical_or, [me == n for n in places])


def tables(live_ref, nb_ref, blocks):
    lives = [live_ref[b] == 1 for b in range(blocks)]
    count = jnp.int32(0)
    first = jnp.int32(0)
    final = jnp.int32(0)
    for b in range(blocks):
        count = count + jnp.where(lives[b], 1, 0)
        first = first + jnp.where(jnp.logical_and(lives[b], nb_ref[0, b] == blocks), b, 0)
        final = final + jnp.where(jnp.logical_and(lives[b], nb_ref[1, b] == blocks), b, 0)
    easts = [nb_ref[1, b] for b in range(blocks)]
    order = [first]
    for _ in range(blocks - 1):
        order.append(jnp.minimum(pick(order[-1], easts), blocks - 1))
    return lives, count, final, order


def window_kernel(
    owners,
    live_hbm, nb_hbm, depth_ref, mom_ref, win_ref,
    loc, edge, got, live_ref, nb_ref,
    in_sem, edge_send, edge_recv,
):
    me = lax.axis_index("tm")
    own = lax.axis_index("space")
    east_owner = lax.rem(own + 1, owners)
    west_owner = lax.rem(own + owners - 1, owners)
    blocks = loc.shape[0]
    west_set, east_set = seams(blocks)
    at_west, at_east = member(me, west_set), member(me, east_set)
    at_seam = jnp.logical_or(at_west, at_east)

    copies = [
        pltpu.make_async_copy(nb_hbm, nb_ref, in_sem.at[0]),
        pltpu.make_async_copy(live_hbm, live_ref, in_sem.at[1]),
        pltpu.make_async_copy(depth_ref, loc.at[:, 0], in_sem.at[2]),
        pltpu.make_async_copy(mom_ref, loc.at[:, 1:3], in_sem.at[3]),
    ]
    for c in copies:
        c.start()
    barrier = pltpu.get_barrier_semaphore()

    @pl.when(at_seam)
    def _():
        for o in (west_owner, east_owner):
            pl.semaphore_signal(barrier, inc=1, device_id=(me, o), device_id_type=MESH)

    for c in copies:
        c.wait()
    lives, count, final, order = tables(live_ref, nb_ref, blocks)

    halo = pltpu.make_async_remote_copy(
        src_ref=edge, dst_ref=got, send_sem=edge_send, recv_sem=edge_recv,
        device_id=(me, jnp.where(at_west, east_owner, west_owner)), device_id_type=MESH,
    )
    edge[...] = loc[jnp.where(at_west, final, order[0])]

    @pl.when(at_seam)
    def _():
        pl.semaphore_wait(barrier, 2)
        halo.start()

    begins = [STARTS[k] - (LANES - STARTS[k + 1] + STARTS[k]) // 2 for k in HOLDS]
    place = pick(me, [begin // LANES for begin in begins])
    offset = pick(me, [begin % LANES for begin in begins])
    lane = lax.broadcasted_iota(jnp.int32, (3, ROWS, LANES), 2)
    left = lane >= offset

    def slot(position):
        return jnp.clip(pick(position, order), 0, blocks - 1)

    win_ref[...] = jnp.where(left, loc[slot(place)], loc[slot(place + 1)])

    @pl.when(at_seam)
    def _():
        halo.wait()
        outside_a = jnp.logical_or(place < 0, place >= count)
        outside_b = place + 1 >= count
        mask = jnp.logical_or(
            jnp.logical_and(left, outside_a), jnp.logical_and(jnp.logical_not(left), outside_b)
        )
        win_ref[...] = jnp.where(mask, got[...], win_ref[...])


def main_kernel(
    n_tm,
    live_hbm, nb_hbm, win_ref, out_ref,
    state, mid, delta, ga, ka, send, recv, run, live_ref, nb_ref,
    in_sem, tm_send, tm_recv,
):
    me = lax.axis_index("tm")
    own = lax.axis_index("space")
    blocks = out_ref.shape[1]
    copies = [
        pltpu.make_async_copy(nb_hbm, nb_ref, in_sem.at[0]),
        pltpu.make_async_copy(live_hbm, live_ref, in_sem.at[1]),
    ]
    for c in copies:
        c.start()
    barrier = pltpu.get_barrier_semaphore()
    for d in range(1, n_tm):
        peer = lax.rem(me + d, n_tm)
        pl.semaphore_signal(barrier, inc=1, device_id=(peer, own), device_id_type=MESH)

    row = lax.broadcasted_iota(jnp.int32, (HALF, LANES), 0)
    for f in range(3):
        for half in range(2):
            rows = win_ref[f, pl.ds(HALF * half, HALF), :]
            for m in (0, n_tm - 1):
                state[f, pl.ds(64 * half + m, HALF, stride=8), :] = rows

    def pair(f, m):
        return state[f, pl.ds(m, HALF, stride=16), :], state[f, pl.ds(m + 8, HALF, stride=16), :]

    def mean(m):
        out = []
        for f in range(3):
            a, b = pair(f, m)
            out.append(0.5 * (a + b))
        return out

    def chain0(n, c):
        g = coarse(c, row)
        for f in range(3):
            ga[n, f] = g[f]
            state[f, pl.ds(n + 1, HALF, stride=16), :] = g[f]
            state[f, pl.ds(n + 9, HALF, stride=16), :] = g[f]
        return g

    c6 = lax.fori_loop(0, n_tm - 2, chain0, mean(0))

    fine(state, mid)

    lane = lax.broadcasted_iota(jnp.int32, (HALF, LANES), 1)
    begin = pick(me, [STARTS[k] for k in HOLDS])
    near = ((lane - begin) & (LANES - 1)) < LANES // 2

    def deliver(n, even, odd):
        for f in range(3):
            send[n, f] = jnp.where(near, even[f], shift(odd[f], LANES // 2))

    def message(n):
        return pltpu.make_async_remote_copy(
            src_ref=send.at[n], dst_ref=recv.at[me], send_sem=tm_send.at[n], recv_sem=tm_recv.at[me],
            device_id=(n, own), device_id_type=MESH,
        )

    def dispatch(n):
        @pl.when(n != me)
        def _():
            message(n).start()

    pairs = [pair(f, 0) for f in range(3)]
    deliver(0, [a for a, _ in pairs], [b for _, b in pairs])
    pl.semaphore_wait(barrier, n_tm - 1)
    dispatch(0)
    for f in range(3):
        for m in (0, n_tm - 1):
            delta[f, pl.ds(m, HALF, stride=8), :] = jnp.zeros((HALF, LANES), jnp.float32)

    def keep1(n, k, g):
        out = []
        for f in range(3):
            ka[n, f] = k[f]
            a, b = pair(f, n)
            d = k[f] - g[f]
            delta[f, pl.ds(n, HALF, stride=8), :] = d
            out.append(d + 0.5 * (a + b))
        return out

    k1, g6 = coarse(mean(0), row), coarse(c6, row)
    for f in range(3):
        ga[n_tm - 2, f] = g6[f]
    c = keep1(1, k1, [ga[1, f] for f in range(3)])

    def chain1(n, c):
        return keep1(n, coarse(c, row), [ga[n, f] for f in range(3)])

    c7 = lax.fori_loop(2, n_tm - 1, chain1, c)
    for f in range(3):
        for j in range(HALF):
            d = delta[f, HALF * j : HALF * j + HALF, :]
            for i in (2 * j, 2 * j + 1):
                state[f, HALF * i : HALF * i + HALF, :] = state[f, HALF * i : HALF * i + HALF, :] + d

    fine(state, mid)
    pairs = [pair(f, 0) for f in range(3)]
    deliver(1, [a for a, _ in pairs], [b for _, b in pairs])
    dispatch(1)

    def keep2(n, k):
        even, odd, out = [], [], []
        for f in range(3):
            a, b = pair(f, n - 1)
            d = k[f] - ka[n, f]
            even.append(a + d)
            odd.append(b + d)
            out.append(d + 0.5 * (a + b))
        return out, even, odd

    k2, k7 = coarse(mean(0), row), coarse(c7, row)
    for f in range(3):
        ka[n_tm - 1, f] = k7[f]

    def chain2(n, carry):
        c, even, odd = carry
        k = coarse(c, row)
        deliver(n - 1, even, odd)
        dispatch(n - 1)
        return keep2(n, k)

    _, even, odd = lax.fori_loop(3, n_tm, chain2, keep2(2, k2))
    deliver(n_tm - 1, even, odd)
    dispatch(n_tm - 1)

    recv[me] = send[me]
    for c in copies:
        c.wait()
    lives, count, _, order = tables(live_ref, nb_ref, blocks)
    for p in range(n_tm):
        @pl.when(p != me)
        def _():
            pltpu.make_async_remote_copy(
                src_ref=send.at[p], dst_ref=recv.at[p], send_sem=tm_send.at[p], recv_sem=tm_recv.at[p],
                device_id=(p, own), device_id_type=MESH,
            ).wait()

    far = (lane + LANES // 2) & (LANES - 1)
    for b in range(blocks):
        lo = LANES * b
        parts = [k for k in range(n_tm) if STARTS[k] < lo + LANES and STARTS[k + 1] > lo]
        for f in range(3):
            even = odd = recv[HOLDS.index(parts[0]), f]
            for k in parts[1:]:
                piece = recv[HOLDS.index(k), f]
                even = jnp.where(lane >= STARTS[k] - lo, piece, even)
                odd = jnp.where(far >= STARTS[k] - lo, piece, odd)
            run[b, f, pl.ds(0, HALF, stride=2), :] = even
            run[b, f, pl.ds(1, HALF, stride=2), :] = shift(odd, LANES // 2)
    for b in range(blocks):
        spot = jnp.int32(0)
        for i in range(1, blocks):
            spot = jnp.where(jnp.logical_and(order[i] == b, count > i), i, spot)
        out_ref[0, b] = jnp.where(lives[b], run[spot], 0.0)


def solution(mesh):
    n_tm, owners = mesh.shape["tm"], mesh.shape["space"]
    blocks = 3
    assert n_tm == len(HOLDS) and STARTS[-1] == blocks * LANES
    f32, i32 = jnp.float32, jnp.int32
    dma = pltpu.SemaphoreType.DMA
    hbm = pl.BlockSpec(memory_space=pltpu.HBM)
    vmem = pl.BlockSpec(memory_space=pltpu.VMEM)
    small = [pltpu.SMEM((blocks,), i32), pltpu.SMEM((2, blocks), i32)]

    def local(water_depth, momentum, slot_live, neighbours):
        sides = neighbours.T
        window = pl.pallas_call(
            functools.partial(window_kernel, owners),
            out_shape=pltpu.VMEM((3, ROWS, LANES), f32),
            in_specs=[hbm] * 4,
            out_specs=vmem,
            scratch_shapes=[
                pltpu.VMEM((blocks, 3, ROWS, LANES), f32),
                pltpu.VMEM((3, ROWS, LANES), f32),
                pltpu.VMEM((3, ROWS, LANES), f32),
                *small,
                dma((4,)),
                dma,
                dma,
            ],
            compiler_params=pltpu.CompilerParams(collective_id=0, has_side_effects=True, vmem_limit_bytes=VMEM_LIMIT),
            name="window",
        )(slot_live, sides, water_depth, momentum)
        return pl.pallas_call(
            functools.partial(main_kernel, n_tm),
            out_shape=pltpu.VMEM((1, blocks, 3, ROWS, LANES), f32),
            in_specs=[hbm, hbm, vmem],
            out_specs=vmem,
            scratch_shapes=[
                pltpu.VMEM((3, HALF * ROWS, LANES), f32),
                pltpu.VMEM((3, HALF * ROWS, LANES), f32),
                pltpu.VMEM((3, HALF * HALF, LANES), f32),
                pltpu.VMEM((n_tm, 3, HALF, LANES), f32),
                pltpu.VMEM((n_tm, 3, HALF, LANES), f32),
                pltpu.VMEM((n_tm, 3, HALF, LANES), f32),
                pltpu.VMEM((n_tm, 3, HALF, LANES), f32),
                pltpu.VMEM((blocks, 3, ROWS, LANES), f32),
                *small,
                dma((2,)),
                dma((n_tm,)),
                dma((n_tm,)),
            ],
            compiler_params=pltpu.CompilerParams(collective_id=1, has_side_effects=True, vmem_limit_bytes=VMEM_LIMIT),
            name="parareal",
        )(slot_live, sides, pltpu.with_memory_space_constraint(window, pltpu.VMEM))

    return jax.shard_map(
        local,
        mesh=mesh,
        in_specs=(P("space", None, None), P("space", None, None, None), P("space"), P("space", None)),
        out_specs=P("tm", "space", None, None, None),
        check_vma=False,
    )
```

```python
import functools

import jax
import jax.numpy as jnp
from jax import lax
from jax.experimental import pallas as pl
from jax.experimental.pallas import tpu as pltpu
from jax.sharding import PartitionSpec as P

SUB = 3
TIME_STEP = 0.15
ROWS = 16
HALF = 8
LANES = 128
REACH = 24
STARTS = (0, 48, 96, 144, 192, 232, 288, 336, 384)
HOLDS = (1, 0, 3, 2, 4, 7, 6, 5)
VMEM_LIMIT = 60 * 1024 * 1024
MESH = pl.DeviceIdType.MESH


def pick(index, values):
    result = values[-1]
    for i in range(len(values) - 2, -1, -1):
        result = jnp.where(index == i, values[i], result)
    return result


def derived(h, m, n):
    r = lax.rsqrt(h)
    c = h * r
    inv = r * r
    u = m * inv
    q = n * inv
    p = 0.5 * h * h
    f1 = m * u + p
    f2 = n * u
    g2 = n * q + p
    sx = jnp.abs(u) + c
    sy = jnp.abs(q) + c
    return f1, f2, g2, sx, sy


def faces(a_v, b_v, a_f, b_f, a_s, b_s):
    top = jnp.maximum(a_s, b_s)
    return [(fa + fb) - top * (vb - va) for va, vb, fa, fb in zip(a_v, b_v, a_f, b_f)]


def shift(x, distance):
    return pltpu.roll(x, (-distance) % LANES, 1)


def rows_part(v, d, row):
    n = v[2]
    f1, f2, g2, sx, sy = d
    up = lambda x: pltpu.roll(x, HALF - 1, 0)
    down = lambda x: pltpu.roll(x, 1, 0)
    vn = [up(x) for x in v]
    wy = faces(v, vn, (n, f2, g2), (vn[2], up(f2), up(g2)), sy, up(sy))
    last, first = row == HALF - 1, row == 0
    sn = sy * n
    zero = jnp.zeros_like(n)
    high = [jnp.where(last, w, x) for w, x in zip((zero, zero, 2.0 * (g2 + sn)), wy)]
    low = [jnp.where(first, w, down(x)) for w, x in zip((zero, zero, 2.0 * (g2 - sn)), wy)]
    return [(-0.5 * TIME_STEP) * (x - y) for x, y in zip(high, low)]


def lane_face(v0, d0, v1, d1):
    return faces(v0, v1, (v0[1], d0[0], d0[1]), (v1[1], d1[0], d1[1]), d0[3], d1[3])


def coarse(v, row):
    a = -0.5 * TIME_STEP * SUB
    at = {o: [shift(x, o) if o else x for x in v] for o in (0, 1, -1, 2, -2)}
    d = {0: derived(*at[0])}
    across = {0: rows_part(at[0], d[0], row)}
    for o in (1, -1):
        across[o] = [shift(y, o) for y in across[0]]
    for o in (1, -1, 2, -2):
        d[o] = derived(*at[o])
    w = {o: lane_face(at[o], d[o], at[o + 1], d[o + 1]) for o in (0, -1, 1, -2)}
    v1 = {
        o: [x + (a * (r - l) + y) for x, r, l, y in zip(at[o], w[o], w[o - 1], across[o])]
        for o in (0, 1, -1)
    }
    e = {o: derived(*v1[o]) for o in (0, 1, -1)}
    across1 = rows_part(v1[0], e[0], row)
    w1 = {o: lane_face(v1[o], e[o], v1[o + 1], e[o + 1]) for o in (0, -1)}
    return [
        0.5 * ((x + x1) + (a * (r - l) + y))
        for x, x1, r, l, y in zip(v, v1[0], w1[0], w1[-1], across1)
    ]


def fine_pass(load, emit, ahead=3):
    v, d, e, w = {}, {}, {}, {}
    low = None
    for t in range(ROWS + 2 * ahead):
        if t < ROWS:
            v[t] = load(t)
            d[t] = derived(*v[t])
            e[t] = [shift(x, 1) for x in v[t]]
        j = t - ahead
        if 0 <= j < ROWS:
            wx = lane_face(v[j], d[j], e[j], derived(*e[j]))
            w[j] = (wx, [shift(y, -1) for y in wx])
        j = t - 2 * ahead
        if 0 <= j < ROWS:
            h, m, n = v[j]
            f1, f2, g2, sx, sy = d[j]
            if j == 0:
                low = [None, None, 2.0 * (g2 - sy * n)]
            if j + 1 < ROWS:
                f1a, f2a, g2a, sxa, sya = d[j + 1]
                high = faces(v[j], v[j + 1], (n, f2, g2), (v[j + 1][2], f2a, g2a), sy, sya)
            else:
                high = [None, None, 2.0 * (g2 + sy * n)]
            diff = []
            for right, left, hi, lo in zip(*w[j], high, low):
                y = right - left
                if hi is not None:
                    y = y + hi
                if lo is not None:
                    y = y - lo
                diff.append(y)
            emit(j, v[j], diff)
            low = high


def fine(state, mid):
    def at(ref, j):
        return [ref[f, HALF * j : HALF * j + HALF, :] for f in range(3)]

    def put(ref, j, v):
        for f in range(3):
            ref[f, HALF * j : HALF * j + HALF, :] = v[f]

    def first(j, v, d):
        put(mid, j, [x - (0.5 * TIME_STEP) * y for x, y in zip(v, d)])

    def second(j, v1, d):
        v = at(state, j)
        put(state, j, [0.5 * (x + y) - (0.25 * TIME_STEP) * z for x, y, z in zip(v, v1, d)])

    def once(i, run):
        def trip(_, carry):
            run()
            return carry

        lax.fori_loop(0, jnp.minimum(i, 0) + 1, trip, 0)

    def step(i, carry):
        once(i, lambda: fine_pass(lambda j: at(state, j), first))
        once(i, lambda: fine_pass(lambda j: at(mid, j), second))
        return carry

    lax.fori_loop(0, SUB, step, 0)


def seams(blocks):
    spans = [(STARTS[k], STARTS[k + 1]) for k in HOLDS]
    west = [n for n, (lo, _) in enumerate(spans) if lo < REACH]
    east = [
        n
        for n, (lo, hi) in enumerate(spans)
        if any(lo < LANES * k < hi + REACH for k in range(1, blocks + 1))
    ]
    assert not set(west) & set(east)
    assert max(hi - lo for lo, hi in spans) + 2 * REACH <= LANES
    return west, east


def member(me, places):
    return functools.reduce(jnp.logical_or, [me == n for n in places])


def tables(live_ref, nb_ref, blocks):
    lives = [live_ref[b] == 1 for b in range(blocks)]
    count = jnp.int32(0)
    first = jnp.int32(0)
    final = jnp.int32(0)
    for b in range(blocks):
        count = count + jnp.where(lives[b], 1, 0)
        first = first + jnp.where(jnp.logical_and(lives[b], nb_ref[0, b] == blocks), b, 0)
        final = final + jnp.where(jnp.logical_and(lives[b], nb_ref[1, b] == blocks), b, 0)
    easts = [nb_ref[1, b] for b in range(blocks)]
    order = [first]
    for _ in range(blocks - 1):
        order.append(jnp.minimum(pick(order[-1], easts), blocks - 1))
    return lives, count, final, order


def window_kernel(
    owners,
    live_hbm, nb_hbm, depth_ref, mom_ref, win_ref,
    loc, edge, got, live_ref, nb_ref,
    in_sem, edge_send, edge_recv,
):
    me = lax.axis_index("tm")
    own = lax.axis_index("space")
    east_owner = lax.rem(own + 1, owners)
    west_owner = lax.rem(own + owners - 1, owners)
    blocks = loc.shape[0]
    west_set, east_set = seams(blocks)
    at_west, at_east = member(me, west_set), member(me, east_set)
    at_seam = jnp.logical_or(at_west, at_east)

    copies = [
        pltpu.make_async_copy(nb_hbm, nb_ref, in_sem.at[0]),
        pltpu.make_async_copy(live_hbm, live_ref, in_sem.at[1]),
        pltpu.make_async_copy(depth_ref, loc.at[:, 0], in_sem.at[2]),
        pltpu.make_async_copy(mom_ref, loc.at[:, 1:3], in_sem.at[3]),
    ]
    for c in copies:
        c.start()
    barrier = pltpu.get_barrier_semaphore()

    @pl.when(at_seam)
    def _():
        for o in (west_owner, east_owner):
            pl.semaphore_signal(barrier, inc=1, device_id=(me, o), device_id_type=MESH)

    for c in copies:
        c.wait()
    lives, count, final, order = tables(live_ref, nb_ref, blocks)

    halo = pltpu.make_async_remote_copy(
        src_ref=edge, dst_ref=got, send_sem=edge_send, recv_sem=edge_recv,
        device_id=(me, jnp.where(at_west, east_owner, west_owner)), device_id_type=MESH,
    )
    edge[...] = loc[jnp.where(at_west, final, order[0])]

    @pl.when(at_seam)
    def _():
        pl.semaphore_wait(barrier, 2)
        halo.start()

    begins = [STARTS[k] - (LANES - STARTS[k + 1] + STARTS[k]) // 2 for k in HOLDS]
    place = pick(me, [begin // LANES for begin in begins])
    offset = pick(me, [begin % LANES for begin in begins])
    lane = lax.broadcasted_iota(jnp.int32, (3, ROWS, LANES), 2)
    left = lane >= offset

    def slot(position):
        return jnp.clip(pick(position, order), 0, blocks - 1)

    win_ref[...] = jnp.where(left, loc[slot(place)], loc[slot(place + 1)])

    @pl.when(at_seam)
    def _():
        halo.wait()
        outside_a = jnp.logical_or(place < 0, place >= count)
        outside_b = place + 1 >= count
        mask = jnp.logical_or(
            jnp.logical_and(left, outside_a), jnp.logical_and(jnp.logical_not(left), outside_b)
        )
        win_ref[...] = jnp.where(mask, got[...], win_ref[...])


def main_kernel(
    n_tm,
    live_hbm, nb_hbm, win_ref, out_ref,
    state, mid, delta, ga, ka, send, recv, run, live_ref, nb_ref,
    in_sem, tm_send, tm_recv,
):
    me = lax.axis_index("tm")
    own = lax.axis_index("space")
    blocks = out_ref.shape[1]
    copies = [
        pltpu.make_async_copy(nb_hbm, nb_ref, in_sem.at[0]),
        pltpu.make_async_copy(live_hbm, live_ref, in_sem.at[1]),
    ]
    for c in copies:
        c.start()
    barrier = pltpu.get_barrier_semaphore()
    for d in range(1, n_tm):
        peer = lax.rem(me + d, n_tm)
        pl.semaphore_signal(barrier, inc=1, device_id=(peer, own), device_id_type=MESH)

    row = lax.broadcasted_iota(jnp.int32, (HALF, LANES), 0)
    for f in range(3):
        for half in range(2):
            rows = win_ref[f, pl.ds(HALF * half, HALF), :]
            for m in (0, n_tm - 1):
                state[f, pl.ds(64 * half + m, HALF, stride=8), :] = rows

    def pair(f, m):
        return state[f, pl.ds(m, HALF, stride=16), :], state[f, pl.ds(m + 8, HALF, stride=16), :]

    def mean(m):
        out = []
        for f in range(3):
            a, b = pair(f, m)
            out.append(0.5 * (a + b))
        return out

    def chain0(n, c):
        g = coarse(c, row)
        for f in range(3):
            ga[n, f] = g[f]
            state[f, pl.ds(n + 1, HALF, stride=16), :] = g[f]
            state[f, pl.ds(n + 9, HALF, stride=16), :] = g[f]
        return g

    c6 = lax.fori_loop(0, n_tm - 2, chain0, mean(0))

    fine(state, mid)

    lane = lax.broadcasted_iota(jnp.int32, (HALF, LANES), 1)
    begin = pick(me, [STARTS[k] for k in HOLDS])
    near = ((lane - begin) & (LANES - 1)) < LANES // 2

    def deliver(n, even, odd):
        for f in range(3):
            send[n, f] = jnp.where(near, even[f], shift(odd[f], LANES // 2))

    def message(n):
        return pltpu.make_async_remote_copy(
            src_ref=send.at[n], dst_ref=recv.at[me], send_sem=tm_send.at[n], recv_sem=tm_recv.at[me],
            device_id=(n, own), device_id_type=MESH,
        )

    def dispatch(n):
        @pl.when(n != me)
        def _():
            message(n).start()

    pairs = [pair(f, 0) for f in range(3)]
    deliver(0, [a for a, _ in pairs], [b for _, b in pairs])
    pl.semaphore_wait(barrier, n_tm - 1)
    dispatch(0)
    for f in range(3):
        for m in (0, n_tm - 1):
            delta[f, pl.ds(m, HALF, stride=8), :] = jnp.zeros((HALF, LANES), jnp.float32)

    def keep1(n, k, g):
        out = []
        for f in range(3):
            ka[n, f] = k[f]
            a, b = pair(f, n)
            d = k[f] - g[f]
            delta[f, pl.ds(n, HALF, stride=8), :] = d
            out.append(d + 0.5 * (a + b))
        return out

    k1, g6 = coarse(mean(0), row), coarse(c6, row)
    for f in range(3):
        ga[n_tm - 2, f] = g6[f]
    c = keep1(1, k1, [ga[1, f] for f in range(3)])

    def chain1(n, c):
        return keep1(n, coarse(c, row), [ga[n, f] for f in range(3)])

    c7 = lax.fori_loop(2, n_tm - 1, chain1, c)
    for f in range(3):
        for j in range(HALF):
            d = delta[f, HALF * j : HALF * j + HALF, :]
            for i in (2 * j, 2 * j + 1):
                state[f, HALF * i : HALF * i + HALF, :] = state[f, HALF * i : HALF * i + HALF, :] + d

    fine(state, mid)
    pairs = [pair(f, 0) for f in range(3)]
    deliver(1, [a for a, _ in pairs], [b for _, b in pairs])
    dispatch(1)

    def keep2(n, k):
        even, odd, out = [], [], []
        for f in range(3):
            a, b = pair(f, n - 1)
            d = k[f] - ka[n, f]
            even.append(a + d)
            odd.append(b + d)
            out.append(d + 0.5 * (a + b))
        return out, even, odd

    k2, k7 = coarse(mean(0), row), coarse(c7, row)
    for f in range(3):
        ka[n_tm - 1, f] = k7[f]

    def chain2(n, carry):
        c, even, odd = carry
        k = coarse(c, row)
        deliver(n - 1, even, odd)
        dispatch(n - 1)
        return keep2(n, k)

    _, even, odd = lax.fori_loop(3, n_tm, chain2, keep2(2, k2))
    deliver(n_tm - 1, even, odd)
    dispatch(n_tm - 1)

    recv[me] = send[me]
    for c in copies:
        c.wait()
    lives, count, _, order = tables(live_ref, nb_ref, blocks)
    for p in range(n_tm):
        @pl.when(p != me)
        def _():
            pltpu.make_async_remote_copy(
                src_ref=send.at[p], dst_ref=recv.at[p], send_sem=tm_send.at[p], recv_sem=tm_recv.at[p],
                device_id=(p, own), device_id_type=MESH,
            ).wait()

    far = (lane + LANES // 2) & (LANES - 1)
    for b in range(blocks):
        lo = LANES * b
        parts = [k for k in range(n_tm) if STARTS[k] < lo + LANES and STARTS[k + 1] > lo]
        for f in range(3):
            even = odd = recv[HOLDS.index(parts[0]), f]
            for k in parts[1:]:
                piece = recv[HOLDS.index(k), f]
                even = jnp.where(lane >= STARTS[k] - lo, piece, even)
                odd = jnp.where(far >= STARTS[k] - lo, piece, odd)
            run[b, f, pl.ds(0, HALF, stride=2), :] = even
            run[b, f, pl.ds(1, HALF, stride=2), :] = shift(odd, LANES // 2)
    for b in range(blocks):
        spot = jnp.int32(0)
        for i in range(1, blocks):
            spot = jnp.where(jnp.logical_and(order[i] == b, count > i), i, spot)
        out_ref[0, b] = jnp.where(lives[b], run[spot], 0.0)


def solution(mesh):
    n_tm, owners = mesh.shape["tm"], mesh.shape["space"]
    blocks = 3
    assert n_tm == len(HOLDS) and STARTS[-1] == blocks * LANES
    f32, i32 = jnp.float32, jnp.int32
    dma = pltpu.SemaphoreType.DMA
    hbm = pl.BlockSpec(memory_space=pltpu.HBM)
    vmem = pl.BlockSpec(memory_space=pltpu.VMEM)
    small = [pltpu.SMEM((blocks,), i32), pltpu.SMEM((2, blocks), i32)]

    def local(water_depth, momentum, slot_live, neighbours):
        sides = neighbours.T
        window = pl.pallas_call(
            functools.partial(window_kernel, owners),
            out_shape=pltpu.VMEM((3, ROWS, LANES), f32),
            in_specs=[hbm] * 4,
            out_specs=vmem,
            scratch_shapes=[
                pltpu.VMEM((blocks, 3, ROWS, LANES), f32),
                pltpu.VMEM((3, ROWS, LANES), f32),
                pltpu.VMEM((3, ROWS, LANES), f32),
                *small,
                dma((4,)),
                dma,
                dma,
            ],
            compiler_params=pltpu.CompilerParams(collective_id=0, has_side_effects=True, vmem_limit_bytes=VMEM_LIMIT),
            name="window",
        )(slot_live, sides, water_depth, momentum)
        return pl.pallas_call(
            functools.partial(main_kernel, n_tm),
            out_shape=pltpu.VMEM((1, blocks, 3, ROWS, LANES), f32),
            in_specs=[hbm, hbm, vmem],
            out_specs=vmem,
            scratch_shapes=[
                pltpu.VMEM((3, HALF * ROWS, LANES), f32),
                pltpu.VMEM((3, HALF * ROWS, LANES), f32),
                pltpu.VMEM((3, HALF * HALF, LANES), f32),
                pltpu.VMEM((n_tm, 3, HALF, LANES), f32),
                pltpu.VMEM((n_tm, 3, HALF, LANES), f32),
                pltpu.VMEM((n_tm, 3, HALF, LANES), f32),
                pltpu.VMEM((n_tm, 3, HALF, LANES), f32),
                pltpu.VMEM((blocks, 3, ROWS, LANES), f32),
                *small,
                dma((2,)),
                dma((n_tm,)),
                dma((n_tm,)),
            ],
            compiler_params=pltpu.CompilerParams(collective_id=1, has_side_effects=True, vmem_limit_bytes=VMEM_LIMIT),
            name="parareal",
        )(slot_live, sides, pltpu.with_memory_space_constraint(window, pltpu.VMEM))

    return jax.shard_map(
        local,
        mesh=mesh,
        in_specs=(P("space", None, None), P("space", None, None, None), P("space"), P("space", None)),
        out_specs=P("tm", "space", None, None, None),
        check_vma=False,
    )
```

```python
import functools

import jax
import jax.numpy as jnp
from jax import lax
from jax.experimental import pallas as pl
from jax.experimental.pallas import tpu as pltpu
from jax.sharding import PartitionSpec as P

SUB = 3
TIME_STEP = 0.15
ROWS = 16
HALF = 8
LANES = 128
REACH = 24
STARTS = (0, 48, 96, 144, 192, 232, 288, 336, 384)
HOLDS = (1, 0, 3, 2, 4, 7, 6, 5)
VMEM_LIMIT = 60 * 1024 * 1024
MESH = pl.DeviceIdType.MESH


def pick(index, values):
    result = values[-1]
    for i in range(len(values) - 2, -1, -1):
        result = jnp.where(index == i, values[i], result)
    return result


def derived(h, m, n):
    r = lax.rsqrt(h)
    c = h * r
    inv = r * r
    u = m * inv
    q = n * inv
    p = 0.5 * h * h
    f1 = m * u + p
    f2 = n * u
    g2 = n * q + p
    sx = jnp.abs(u) + c
    sy = jnp.abs(q) + c
    return f1, f2, g2, sx, sy


def faces(a_v, b_v, a_f, b_f, a_s, b_s):
    top = jnp.maximum(a_s, b_s)
    return [(fa + fb) - top * (vb - va) for va, vb, fa, fb in zip(a_v, b_v, a_f, b_f)]


def shift(x, distance):
    return pltpu.roll(x, (-distance) % LANES, 1)


def rows_part(v, d, row):
    n = v[2]
    f1, f2, g2, sx, sy = d
    up = lambda x: pltpu.roll(x, HALF - 1, 0)
    down = lambda x: pltpu.roll(x, 1, 0)
    vn = [up(x) for x in v]
    wy = faces(v, vn, (n, f2, g2), (vn[2], up(f2), up(g2)), sy, up(sy))
    last, first = row == HALF - 1, row == 0
    sn = sy * n
    zero = jnp.zeros_like(n)
    high = [jnp.where(last, w, x) for w, x in zip((zero, zero, 2.0 * (g2 + sn)), wy)]
    low = [jnp.where(first, w, down(x)) for w, x in zip((zero, zero, 2.0 * (g2 - sn)), wy)]
    return [(-0.5 * TIME_STEP) * (x - y) for x, y in zip(high, low)]


def lane_face(v0, d0, v1, d1):
    return faces(v0, v1, (v0[1], d0[0], d0[1]), (v1[1], d1[0], d1[1]), d0[3], d1[3])


def coarse(v, row):
    a = -0.5 * TIME_STEP * SUB
    at = {o: [shift(x, o) if o else x for x in v] for o in (0, 1, -1, 2, -2)}
    d = {0: derived(*at[0])}
    across = {0: rows_part(at[0], d[0], row)}
    for o in (1, -1):
        across[o] = [shift(y, o) for y in across[0]]
    for o in (1, -1, 2, -2):
        d[o] = derived(*at[o])
    w = {o: lane_face(at[o], d[o], at[o + 1], d[o + 1]) for o in (0, -1, 1, -2)}
    v1 = {
        o: [x + (a * (r - l) + y) for x, r, l, y in zip(at[o], w[o], w[o - 1], across[o])]
        for o in (0, 1, -1)
    }
    e = {o: derived(*v1[o]) for o in (0, 1, -1)}
    across1 = rows_part(v1[0], e[0], row)
    w1 = {o: lane_face(v1[o], e[o], v1[o + 1], e[o + 1]) for o in (0, -1)}
    return [
        0.5 * ((x + x1) + (a * (r - l) + y))
        for x, x1, r, l, y in zip(v, v1[0], w1[0], w1[-1], across1)
    ]


def fine_pass(load, emit, ahead=3):
    v, d, e, w = {}, {}, {}, {}
    low = None
    for t in range(ROWS + 2 * ahead):
        if t < ROWS:
            v[t] = load(t)
            d[t] = derived(*v[t])
            e[t] = [shift(x, 1) for x in v[t]]
        j = t - ahead
        if 0 <= j < ROWS:
            wx = lane_face(v[j], d[j], e[j], derived(*e[j]))
            w[j] = (wx, [shift(y, -1) for y in wx])
        j = t - 2 * ahead
        if 0 <= j < ROWS:
            h, m, n = v[j]
            f1, f2, g2, sx, sy = d[j]
            if j == 0:
                low = [None, None, 2.0 * (g2 - sy * n)]
            if j + 1 < ROWS:
                f1a, f2a, g2a, sxa, sya = d[j + 1]
                high = faces(v[j], v[j + 1], (n, f2, g2), (v[j + 1][2], f2a, g2a), sy, sya)
            else:
                high = [None, None, 2.0 * (g2 + sy * n)]
            diff = []
            for right, left, hi, lo in zip(*w[j], high, low):
                y = right - left
                if hi is not None:
                    y = y + hi
                if lo is not None:
                    y = y - lo
                diff.append(y)
            emit(j, v[j], diff)
            low = high


def fine(state, mid):
    def at(ref, j):
        return [ref[f, HALF * j : HALF * j + HALF, :] for f in range(3)]

    def put(ref, j, v):
        for f in range(3):
            ref[f, HALF * j : HALF * j + HALF, :] = v[f]

    def first(j, v, d):
        put(mid, j, [x - (0.5 * TIME_STEP) * y for x, y in zip(v, d)])

    def second(j, v1, d):
        v = at(state, j)
        put(state, j, [0.5 * (x + y) - (0.25 * TIME_STEP) * z for x, y, z in zip(v, v1, d)])

    def once(i, run):
        def trip(_, carry):
            run()
            return carry

        lax.fori_loop(0, jnp.minimum(i, 0) + 1, trip, 0)

    def step(i, carry):
        once(i, lambda: fine_pass(lambda j: at(state, j), first))
        once(i, lambda: fine_pass(lambda j: at(mid, j), second))
        return carry

    lax.fori_loop(0, SUB, step, 0)


def seams(blocks):
    spans = [(STARTS[k], STARTS[k + 1]) for k in HOLDS]
    west = [n for n, (lo, _) in enumerate(spans) if lo < REACH]
    east = [
        n
        for n, (lo, hi) in enumerate(spans)
        if any(lo < LANES * k < hi + REACH for k in range(1, blocks + 1))
    ]
    assert not set(west) & set(east)
    assert max(hi - lo for lo, hi in spans) + 2 * REACH <= LANES
    return west, east


def member(me, places):
    return functools.reduce(jnp.logical_or, [me == n for n in places])


def tables(live_ref, nb_ref, blocks):
    lives = [live_ref[b] == 1 for b in range(blocks)]
    count = jnp.int32(0)
    first = jnp.int32(0)
    final = jnp.int32(0)
    for b in range(blocks):
        count = count + jnp.where(lives[b], 1, 0)
        first = first + jnp.where(jnp.logical_and(lives[b], nb_ref[0, b] == blocks), b, 0)
        final = final + jnp.where(jnp.logical_and(lives[b], nb_ref[1, b] == blocks), b, 0)
    easts = [nb_ref[1, b] for b in range(blocks)]
    order = [first]
    for _ in range(blocks - 1):
        order.append(jnp.minimum(pick(order[-1], easts), blocks - 1))
    return lives, count, final, order


def window_kernel(
    owners,
    live_hbm, nb_hbm, depth_ref, mom_ref, win_ref,
    loc, edge, got, live_ref, nb_ref,
    in_sem, edge_send, edge_recv,
):
    me = lax.axis_index("tm")
    own = lax.axis_index("space")
    east_owner = lax.rem(own + 1, owners)
    west_owner = lax.rem(own + owners - 1, owners)
    blocks = loc.shape[0]
    west_set, east_set = seams(blocks)
    at_west, at_east = member(me, west_set), member(me, east_set)
    at_seam = jnp.logical_or(at_west, at_east)

    copies = [
        pltpu.make_async_copy(nb_hbm, nb_ref, in_sem.at[0]),
        pltpu.make_async_copy(live_hbm, live_ref, in_sem.at[1]),
        pltpu.make_async_copy(depth_ref, loc.at[:, 0], in_sem.at[2]),
        pltpu.make_async_copy(mom_ref, loc.at[:, 1:3], in_sem.at[3]),
    ]
    for c in copies:
        c.start()
    barrier = pltpu.get_barrier_semaphore()

    @pl.when(at_seam)
    def _():
        for o in (west_owner, east_owner):
            pl.semaphore_signal(barrier, inc=1, device_id=(me, o), device_id_type=MESH)

    for c in copies[:2]:
        c.wait()
    lives, count, final, order = tables(live_ref, nb_ref, blocks)
    for c in copies[2:]:
        c.wait()

    halo = pltpu.make_async_remote_copy(
        src_ref=edge, dst_ref=got, send_sem=edge_send, recv_sem=edge_recv,
        device_id=(me, jnp.where(at_west, east_owner, west_owner)), device_id_type=MESH,
    )
    edge[...] = loc[jnp.where(at_west, final, order[0])]

    @pl.when(at_seam)
    def _():
        pl.semaphore_wait(barrier, 2)
        halo.start()

    begins = [STARTS[k] - (LANES - STARTS[k + 1] + STARTS[k]) // 2 for k in HOLDS]
    place = pick(me, [begin // LANES for begin in begins])
    offset = pick(me, [begin % LANES for begin in begins])
    lane = lax.broadcasted_iota(jnp.int32, (3, ROWS, LANES), 2)
    left = lane >= offset

    def slot(position):
        return jnp.clip(pick(position, order), 0, blocks - 1)

    win_ref[...] = jnp.where(left, loc[slot(place)], loc[slot(place + 1)])

    @pl.when(at_seam)
    def _():
        halo.wait()
        outside_a = jnp.logical_or(place < 0, place >= count)
        outside_b = place + 1 >= count
        mask = jnp.logical_or(
            jnp.logical_and(left, outside_a), jnp.logical_and(jnp.logical_not(left), outside_b)
        )
        win_ref[...] = jnp.where(mask, got[...], win_ref[...])


def main_kernel(
    n_tm,
    live_hbm, nb_hbm, win_ref, out_ref,
    state, mid, delta, ga, ka, send, recv, run, live_ref, nb_ref,
    in_sem, tm_send, tm_recv,
):
    me = lax.axis_index("tm")
    own = lax.axis_index("space")
    blocks = out_ref.shape[1]
    copies = [
        pltpu.make_async_copy(nb_hbm, nb_ref, in_sem.at[0]),
        pltpu.make_async_copy(live_hbm, live_ref, in_sem.at[1]),
    ]
    for c in copies:
        c.start()
    barrier = pltpu.get_barrier_semaphore()
    for d in range(1, n_tm):
        peer = lax.rem(me + d, n_tm)
        pl.semaphore_signal(barrier, inc=1, device_id=(peer, own), device_id_type=MESH)

    row = lax.broadcasted_iota(jnp.int32, (HALF, LANES), 0)
    for f in range(3):
        for half in range(2):
            rows = win_ref[f, pl.ds(HALF * half, HALF), :]
            for m in (0, n_tm - 1):
                state[f, pl.ds(64 * half + m, HALF, stride=8), :] = rows

    def pair(f, m):
        return state[f, pl.ds(m, HALF, stride=16), :], state[f, pl.ds(m + 8, HALF, stride=16), :]

    def mean(m):
        out = []
        for f in range(3):
            a, b = pair(f, m)
            out.append(0.5 * (a + b))
        return out

    def chain0(n, c):
        g = coarse(c, row)
        for f in range(3):
            ga[n, f] = g[f]
            state[f, pl.ds(n + 1, HALF, stride=16), :] = g[f]
            state[f, pl.ds(n + 9, HALF, stride=16), :] = g[f]
        return g

    c6 = mean(0)
    for n in range(n_tm - 2):
        c6 = chain0(n, c6)

    fine(state, mid)

    lane = lax.broadcasted_iota(jnp.int32, (HALF, LANES), 1)
    begin = pick(me, [STARTS[k] for k in HOLDS])
    near = ((lane - begin) & (LANES - 1)) < LANES // 2

    def deliver(n, even, odd):
        for f in range(3):
            send[n, f] = jnp.where(near, even[f], shift(odd[f], LANES // 2))

    def message(n):
        return pltpu.make_async_remote_copy(
            src_ref=send.at[n], dst_ref=recv.at[me], send_sem=tm_send.at[n], recv_sem=tm_recv.at[me],
            device_id=(n, own), device_id_type=MESH,
        )

    def dispatch(n):
        @pl.when(n != me)
        def _():
            message(n).start()

    pairs = [pair(f, 0) for f in range(3)]
    deliver(0, [a for a, _ in pairs], [b for _, b in pairs])
    pl.semaphore_wait(barrier, n_tm - 1)
    dispatch(0)
    for f in range(3):
        for m in (0, n_tm - 1):
            delta[f, pl.ds(m, HALF, stride=8), :] = jnp.zeros((HALF, LANES), jnp.float32)

    def keep1(n, k, g):
        out = []
        for f in range(3):
            ka[n, f] = k[f]
            a, b = pair(f, n)
            d = k[f] - g[f]
            delta[f, pl.ds(n, HALF, stride=8), :] = d
            out.append(d + 0.5 * (a + b))
        return out

    k1, g6 = coarse(mean(0), row), coarse(c6, row)
    for f in range(3):
        ga[n_tm - 2, f] = g6[f]
    c = keep1(1, k1, [ga[1, f] for f in range(3)])

    def chain1(n, c):
        return keep1(n, coarse(c, row), [ga[n, f] for f in range(3)])

    c7 = c
    for n in range(2, n_tm - 1):
        c7 = chain1(n, c7)
    for f in range(3):
        for j in range(HALF):
            d = delta[f, HALF * j : HALF * j + HALF, :]
            for i in (2 * j, 2 * j + 1):
                state[f, HALF * i : HALF * i + HALF, :] = state[f, HALF * i : HALF * i + HALF, :] + d

    fine(state, mid)
    pairs = [pair(f, 0) for f in range(3)]
    deliver(1, [a for a, _ in pairs], [b for _, b in pairs])
    dispatch(1)

    def keep2(n, k):
        even, odd, out = [], [], []
        for f in range(3):
            a, b = pair(f, n - 1)
            d = k[f] - ka[n, f]
            even.append(a + d)
            odd.append(b + d)
            out.append(d + 0.5 * (a + b))
        return out, even, odd

    k2, k7 = coarse(mean(0), row), coarse(c7, row)
    for f in range(3):
        ka[n_tm - 1, f] = k7[f]

    def chain2(n, carry):
        c, even, odd = carry
        k = coarse(c, row)
        deliver(n - 1, even, odd)
        dispatch(n - 1)
        return keep2(n, k)

    _, even, odd = lax.fori_loop(3, n_tm, chain2, keep2(2, k2))
    deliver(n_tm - 1, even, odd)
    dispatch(n_tm - 1)

    recv[me] = send[me]
    for c in copies:
        c.wait()
    lives, count, _, order = tables(live_ref, nb_ref, blocks)
    def other(p):
        return pltpu.make_async_remote_copy(
            src_ref=send.at[p], dst_ref=recv.at[p], send_sem=tm_send.at[p], recv_sem=tm_recv.at[p],
            device_id=(p, own), device_id_type=MESH,
        )

    for p in sorted(range(n_tm), key=lambda n: n % 2):
        @pl.when(p != me)
        def _():
            other(p).wait_recv()

    far = (lane + LANES // 2) & (LANES - 1)
    for b in range(blocks):
        lo = LANES * b
        parts = [k for k in range(n_tm) if STARTS[k] < lo + LANES and STARTS[k + 1] > lo]
        for f in range(3):
            even = odd = recv[HOLDS.index(parts[0]), f]
            for k in parts[1:]:
                piece = recv[HOLDS.index(k), f]
                even = jnp.where(lane >= STARTS[k] - lo, piece, even)
                odd = jnp.where(far >= STARTS[k] - lo, piece, odd)
            run[b, f, pl.ds(0, HALF, stride=2), :] = even
            run[b, f, pl.ds(1, HALF, stride=2), :] = shift(odd, LANES // 2)
    for b in range(blocks):
        spot = jnp.int32(0)
        for i in range(1, blocks):
            spot = jnp.where(jnp.logical_and(order[i] == b, count > i), i, spot)
        out_ref[0, b] = jnp.where(lives[b], run[spot], 0.0)
    for p in range(n_tm):
        @pl.when(p != me)
        def _():
            other(p).wait_send()


def solution(mesh):
    n_tm, owners = mesh.shape["tm"], mesh.shape["space"]
    blocks = 3
    assert n_tm == len(HOLDS) and STARTS[-1] == blocks * LANES
    f32, i32 = jnp.float32, jnp.int32
    dma = pltpu.SemaphoreType.DMA
    hbm = pl.BlockSpec(memory_space=pltpu.HBM)
    vmem = pl.BlockSpec(memory_space=pltpu.VMEM)
    small = [pltpu.SMEM((blocks,), i32), pltpu.SMEM((2, blocks), i32)]

    def local(water_depth, momentum, slot_live, neighbours):
        sides = neighbours.T
        window = pl.pallas_call(
            functools.partial(window_kernel, owners),
            out_shape=pltpu.VMEM((3, ROWS, LANES), f32),
            in_specs=[hbm] * 4,
            out_specs=vmem,
            scratch_shapes=[
                pltpu.VMEM((blocks, 3, ROWS, LANES), f32),
                pltpu.VMEM((3, ROWS, LANES), f32),
                pltpu.VMEM((3, ROWS, LANES), f32),
                *small,
                dma((4,)),
                dma,
                dma,
            ],
            compiler_params=pltpu.CompilerParams(collective_id=0, has_side_effects=True, vmem_limit_bytes=VMEM_LIMIT),
            name="window",
        )(slot_live, sides, water_depth, momentum)
        return pl.pallas_call(
            functools.partial(main_kernel, n_tm),
            out_shape=pltpu.VMEM((1, blocks, 3, ROWS, LANES), f32),
            in_specs=[hbm, hbm, vmem],
            out_specs=vmem,
            scratch_shapes=[
                pltpu.VMEM((3, HALF * ROWS, LANES), f32),
                pltpu.VMEM((3, HALF * ROWS, LANES), f32),
                pltpu.VMEM((3, HALF * HALF, LANES), f32),
                pltpu.VMEM((n_tm, 3, HALF, LANES), f32),
                pltpu.VMEM((n_tm, 3, HALF, LANES), f32),
                pltpu.VMEM((n_tm, 3, HALF, LANES), f32),
                pltpu.VMEM((n_tm, 3, HALF, LANES), f32),
                pltpu.VMEM((blocks, 3, ROWS, LANES), f32),
                *small,
                dma((2,)),
                dma((n_tm,)),
                dma((n_tm,)),
            ],
            compiler_params=pltpu.CompilerParams(collective_id=1, has_side_effects=True, vmem_limit_bytes=VMEM_LIMIT),
            name="parareal",
        )(slot_live, sides, pltpu.with_memory_space_constraint(window, pltpu.VMEM))

    return jax.shard_map(
        local,
        mesh=mesh,
        in_specs=(P("space", None, None), P("space", None, None, None), P("space"), P("space", None)),
        out_specs=P("tm", "space", None, None, None),
        check_vma=False,
    )
```
